256 devices in a mesh: row: 16 (over x, z_hi, core), col: 16 (over z_lo, y).
Axes of the slice: x: 4, y: 4, z: 8 (z_hi: 2, z_lo: 4; z = z_hi * 4 + z_lo), core: 2. Of those that a mesh axis runs over, the one named last changes fastest.
Arguments:
- state: float32 [512, 65536], P(None, ('row', 'col')), may hold values from -6 to 6
- obs_index: int32 [2, 512], replicated, may hold values from 0 to 65535
- obs_values: float32 [2, 512], replicated, may hold values from -6 to 6
- obs_var: float32 [2, 512], replicated, may hold values from 0.3 to 3
- noise: float32 [2, 512, 512], P(None, None, 'col'), may hold values from -6 to 6
Outputs:
- analysis: float32 [512, 65536], P(None, ('row', 'col'))
The draws below stay inside these ranges and needn't reach their ends.
All inputs are finite; a program needn't handle non-finite values.
Results may differ from the reference program's by a relative error of at most 0.0001.
Values sent between devices are 32-bit elements; how exact they have to be, the bound alone decides.
No kernel may reach another device: no remote copies, remote signals or barrier semaphores. Data moves between devices by JAX's collectives and lax.ppermute only.
A program may use at most 64 MiB of HBM per device.

```python
import math
import jax
import jax.numpy as jnp
from jax import lax

MEMBERS = 512
NOBS = 512
BATCHES = 2
RADIUS = 64
ROWS_DEV = 256
NROWS = 65536
BIN_ROWS = 256
DEVICES = 256


def touch_ends(drawn, stream_key, least, largest):
    longest = drawn.shape.index(max(drawn.shape))
    spots = []
    for shift in (0, 1):
        where = [jax.random.randint(jax.random.fold_in(stream_key, axis), (), 0, length) for axis, length in enumerate(drawn.shape)]
        where[longest] = (where[longest] + shift) % drawn.shape[longest]
        spots.append(tuple(where))
    return drawn.at[spots[0]].set(least).at[spots[1]].set(largest)


def level_of(key, extent, split, least, high):
    def one(dim, blocks):
        heights = jax.random.uniform(jax.random.fold_in(jax.random.fold_in(key, 6), dim), (blocks,), jnp.float32, least / len(split), high / len(split))
        return jnp.repeat(jnp.exp(heights), extent[dim] // blocks).reshape((-1,) + (1,) * (len(extent) - dim - 1))

    factor_of = one(*split[0])
    for cut in split[1:]:
        factor_of = factor_of * one(*cut)
    return factor_of


def centred(rng, shape, spread, reach, shards=(), held_as=jnp.bfloat16):
    entries = spread * jax.random.normal(rng, shape, jnp.float32)
    if shards:
        entries = entries * level_of(rng, shape, shards, -0.22, 0.18)
    return jnp.clip(entries, -reach, reach).astype(held_as)


def setup_inputs(seed: int = 0) -> dict:
    key_of = jax.random.split(jax.random.key(seed), 6)
    return {
        "state": centred(key_of[0], (MEMBERS, NROWS), 1.0, 6.0, ((1, 256),), jnp.float32),
        "obs_index": touch_ends(jax.random.randint(key_of[1], (BATCHES, NOBS), 0, NROWS), jax.random.fold_in(key_of[1], 1), 0, NROWS - 1).astype(jnp.int32),
        "obs_values": centred(key_of[2], (BATCHES, NOBS), 1.0, 6.0, (), jnp.float32),
        "obs_var": jnp.clip(jnp.exp(jax.random.uniform(key_of[3], (BATCHES, NOBS), jnp.float32, math.log(0.3), math.log(3.0))), 0.3, 3.0),
        "noise": centred(key_of[4], (BATCHES, NOBS, MEMBERS), 1.0, 6.0, ((2, 16),), jnp.float32),
    }


precise = lax.Precision.HIGHEST

def taper_between(first_pos, second_pos):
    distance = (first_pos[:, None] - second_pos[None, :]).astype(jnp.float32)
    scaled = distance / RADIUS
    return jnp.exp(-0.5 * scaled * scaled)

def cholesky_solve(factor, right_side):
    forward = lax.linalg.triangular_solve(factor, right_side, left_side=True, lower=True)
    return lax.linalg.triangular_solve(factor, forward, left_side=True, lower=True, transpose_a=True)

def reference(state, obs_index, obs_values, obs_var, noise):
    norming = 1.0 / (MEMBERS - 1)
    positions = (jnp.arange(NROWS, dtype=jnp.int32) // BIN_ROWS).reshape(DEVICES, ROWS_DEV)
    for batch_index in range(BATCHES):
        obs_rows = obs_index[batch_index].astype(jnp.int32)
        observed = jnp.take(state, obs_rows, axis=1).T
        anomaly_obs = observed - lax.optimization_barrier(jnp.mean(observed, axis=1, keepdims=True))
        obs_pos = obs_rows // BIN_ROWS
        product = jnp.dot(anomaly_obs, anomaly_obs.T, precision=precise)
        covar = taper_between(obs_pos, obs_pos) * product * norming + jnp.diag(obs_var[batch_index])
        innovation = obs_values[batch_index][:, None] + jnp.sqrt(obs_var[batch_index])[:, None] * noise[batch_index] - observed
        factor = jnp.linalg.cholesky(covar)
        solved = cholesky_solve(factor, innovation)
        anomaly_state = state - lax.optimization_barrier(jnp.mean(state, axis=0, keepdims=True))
        tiles = anomaly_state.reshape(MEMBERS, DEVICES, ROWS_DEV).transpose(1, 0, 2)

        def update_tile(operands):
            state_tile, tile_pos = operands
            cross_cov = jnp.dot(anomaly_obs, state_tile, precision=precise) * norming
            weighted = taper_between(obs_pos, tile_pos) * cross_cov
            return jnp.dot(solved.T, weighted, precision=precise)
        increment = lax.map(update_tile, (tiles, positions))
        state = state + increment.transpose(1, 0, 2).reshape(MEMBERS, NROWS)
    return state
```

```python
import functools

import jax
import jax.numpy as jnp
from jax import lax
from jax.experimental import pallas as pl
from jax.experimental.pallas import tpu as pltpu
from jax.sharding import Mesh
from jax.sharding import PartitionSpec as P


POSITIONS = 256
RADIUS = 64
ROW = ("x", "zh", "core")
COL = ("zl", "y")
ROW_COL = ROW + COL
SLOTS = 4

f32 = jnp.float32
bf16 = jnp.bfloat16
i32 = jnp.int32


def nn(a, b):
    return lax.dot_general(a, b, (((1,), (0,)), ((), ())), preferred_element_type=f32)


def nt(a, b):
    return lax.dot_general(a, b, (((1,), (1,)), ((), ())), preferred_element_type=f32)


def split2(x):
    high = x.astype(bf16)
    return high, (x - high.astype(f32)).astype(bf16)


def split3(x):
    high = x.astype(bf16)
    rest = x - high.astype(f32)
    middle = rest.astype(bf16)
    return high, middle, (rest - middle.astype(f32)).astype(bf16)


def one_hot(mask):
    return jnp.where(mask, 1.0, 0.0).astype(bf16)


def exact_nn(hot, x):
    high, middle, low = split3(x)
    return nn(hot, high) + nn(hot, middle) + nn(hot, low)


def exact_nt(hot, x):
    high, middle, low = split3(x)
    return nt(hot, high) + nt(hot, middle) + nt(hot, low)


def exact_tn(x, hot):
    high, middle, low = split3(x)
    return nt(high, hot) + nt(middle, hot) + nt(low, hot)


def column_of(row):
    return jnp.broadcast_to(row, (128, row.shape[1])).T[:, 0:1]


def iota(shape, dim):
    return lax.broadcasted_iota(i32, shape, dim)


def shift_of(value):
    assert value & (value - 1) == 0
    return value.bit_length() - 1


def right(value, bits):
    return lax.shift_right_logical(value, jnp.full(value.shape, bits, i32))


def order_of(rows, tile_rows, cols, obs):
    tile = right(rows, shift_of(tile_rows))
    key = (tile * obs + iota((1, obs), 1)).astype(f32)
    rank = jnp.sum(jnp.where(column_of(key) < key, 1.0, 0.0), axis=0, keepdims=True)
    rank = rank.astype(i32)
    return tile, rank


def prep_kernel(dims, where_ref, index_ref, values_ref, var_ref, state_ref, noise_ref,
                send_ref, par_ref, noise_out_ref):
    tile_rows, bin_rows, cols = dims
    members, rows_dev = state_ref.shape
    batches, obs = index_ref.shape
    my_tile, first, turn = where_ref[0], where_ref[1], where_ref[2]
    slots = send_ref.shape[0]
    per_col = slots // cols
    pick = jnp.zeros((slots, rows_dev), f32)
    for b in range(batches):
        rows = index_ref[b:b + 1, :]
        tile, rank = order_of(rows, tile_rows, cols, obs)
        col = rank & (cols - 1)
        placed = col * (obs // cols) + right(rank, shift_of(cols))
        start = jnp.sum(jnp.where(tile < my_tile, 1.0, 0.0), axis=1, keepdims=True).astype(i32)
        base = start + ((col - start) & (cols - 1))
        turn_slot = right(rank - base + 16 * cols * obs, shift_of(cols)) - 16 * obs - turn * SLOTS
        local = rows - first
        inside = (local >= 0) & (local < rows_dev) & (turn_slot >= 0) & (turn_slot < SLOTS)
        slot = jnp.where(inside, col * per_col + b * SLOTS + turn_slot, -1)
        pick += nt(one_hot(iota((slots, obs), 0) == slot),
                   one_hot(iota((rows_dev, obs), 0) == local))
        if par_ref is not None:
            hot = one_hot(iota((obs, obs), 0) == placed)
            par = jnp.concatenate(
                [right(rows, shift_of(bin_rows)).astype(f32), values_ref[b:b + 1, :],
                 var_ref[b:b + 1, :], jnp.zeros((1, obs), f32)], axis=0)
            par = jnp.concatenate([par, par], axis=0)
            par_ref[4 * b:4 * b + 4, :] = exact_tn(par, hot)[0:4]
            noise_out_ref[b] = exact_tn(noise_ref[b].T, hot)
    send_ref[...] = exact_nt(pick.astype(bf16), state_ref[...])


def send_kernel(dims, where_ref, index_ref, state_ref, send_ref):
    prep_kernel(dims, where_ref, index_ref, None, None, state_ref, None, send_ref, None, None)


def place_kernel(dims, where_ref, index_ref, slots_ref, out_ref):
    tile_rows, cols, sizes = dims
    batches, obs = index_ref.shape
    slots = slots_ref.shape[0]
    my_col, turn = where_ref[0], where_ref[1]
    mine = [where_ref[2 + k] for k in range(3)]
    half = out_ref.shape[0] // batches
    p = iota((slots, 1), 0)
    block = right(p, shift_of(batches * SLOTS))
    batch = right(p, shift_of(SLOTS)) & (batches - 1)
    slot = (p & (SLOTS - 1)) + turn * SLOTS
    nx, nz, nc = sizes
    block_z = block & (nz - 1)
    block_x = right(block, shift_of(nz)) & (nx - 1)
    block_c = right(block, shift_of(nz * nx))
    tile_p = (((mine[0] - block_x) & (nx - 1)) * nz + ((mine[1] - block_z) & (nz - 1))) * nc
    tile_p = tile_p + ((mine[2] - block_c) & (nc - 1))
    start = jnp.zeros((slots, 1), i32)
    end = jnp.zeros((slots, 1), i32)
    for b in range(batches):
        tile = right(index_ref[b:b + 1, :], shift_of(tile_rows))
        before = jnp.sum(jnp.where(tile < tile_p, 1.0, 0.0), axis=1, keepdims=True).astype(i32)
        through = jnp.sum(jnp.where(tile <= tile_p, 1.0, 0.0), axis=1, keepdims=True).astype(i32)
        start = jnp.where(batch == b, before, start)
        end = jnp.where(batch == b, through, end)
    rank = start + ((my_col - start) & (cols - 1)) + slot * cols
    j = right(rank - my_col, shift_of(cols)) - mine[2] * half
    target = jnp.where((rank < end) & (j >= 0) & (j < half), batch * half + j, -1)
    wide = 128
    hot = jnp.where(iota((slots, wide), 1) == target, 1.0, 0.0).T.astype(bf16)
    out_ref[...] = exact_nn(hot[0:out_ref.shape[0]], slots_ref[...])


def taper(first, second):
    scaled = (first - second) * (1.0 / RADIUS)
    return jnp.exp(-0.5 * scaled * scaled)


def main_kernel(dims, where_ref, par_ref, o0a, o0b, o1a, o1b, na, nb, x_ref, out_ref,
                o0, o1, n0, n1, gram, left, high, middle, low, s_high, s_low, xb, eh, el, rb):
    bin_rows, nzl, ny = dims
    zl, y, core, first = [where_ref[k] for k in range(4)]
    obs, members = o0.shape
    rows_dev = x_ref.shape[1]
    unit = 16
    pieces = o0a.shape[0] // (nzl * ny)
    for part, sources in enumerate(((o0a, o1a, na), (o0b, o1b, nb))):
        half = core if part == 0 else 1 - core
        for dy in range(ny):
            for dz in range(nzl):
                at = ((((zl - dz) & (nzl - 1)) * ny + ((y - dy) & (ny - 1))) * 2 + half) * unit
                at = pl.multiple_of(at, unit)
                k = dy * nzl + dz
                o0[pl.ds(at, unit), :] = sources[0][k * unit:(k + 1) * unit, :]
                o1[pl.ds(at, unit), :] = sources[1][k * unit:(k + 1) * unit, :]
                n0[pl.ds(at, unit), :] = sources[2][2 * k * unit:(2 * k + 1) * unit, :]
                n1[pl.ds(at, unit), :] = sources[2][(2 * k + 1) * unit:(2 * k + 2) * unit, :]
    norming = 1.0 / (members - 1)
    par_t = jnp.concatenate([par_ref[...], jnp.zeros((120, obs), f32)], axis=0).T
    pos_dev = right(first + iota((1, rows_dev), 1), shift_of(bin_rows)).astype(f32)
    eye = iota((obs, obs), 0) == iota((obs, obs), 1)

    def invert(b, o_ref):
        pos_r, var_r = par_ref[4 * b:4 * b + 1, :], par_ref[4 * b + 2:4 * b + 3, :]
        pos_c = par_t[:, 4 * b:4 * b + 1]
        o = o_ref[...]
        anomaly = o - jnp.mean(o, axis=1, keepdims=True)
        h, m, l = split3(anomaly)
        high[...] = h
        middle[...] = m
        low[...] = l
        left[...] = nt(high[...], middle[...]) + nt(high[...], low[...])
        product = nt(high[...], high[...]) + nt(middle[...], middle[...]) + left[...] + left[...].T
        covar = taper(pos_c, pos_r) * product * norming + jnp.where(eye, var_r, 0.0)
        diag_r = jnp.sum(jnp.where(eye, covar, 0.0), axis=0, keepdims=True)
        diag_c = jnp.sum(jnp.where(eye, covar, 0.0), axis=1, keepdims=True)
        scale_r, scale_c = lax.rsqrt(diag_r), lax.rsqrt(diag_c)
        scaled = covar * scale_c * scale_r
        gram[...] = scaled
        sh, sl = split2(scaled)
        s_high[...] = sh
        s_low[...] = sl
        square = nn(s_high[...], s_high[...])
        bound = jnp.max(jnp.sum(jnp.abs(square), axis=1, keepdims=True), axis=0, keepdims=True)
        upper = jnp.sqrt(bound) * 1.01
        lower = jnp.min(var_r * scale_r * scale_r, axis=1, keepdims=True)
        alpha = 2.0 / (upper + lower)

        def widen(low_end):
            image = low_end * (2.0 - low_end)
            return 2.0 / (1.0 + image), image

        factor, image = widen(alpha * lower)
        ident = jnp.where(eye, 1.0, 0.0)
        xb[...] = (factor * alpha * (2.0 * ident - alpha * gram[...])).astype(bf16)
        rb[...] = (ident - factor * (2.0 * alpha * gram[...] - alpha * alpha * square)).astype(bf16)
        low_end = factor * image
        for step in range(3):
            factor, image = widen(low_end)
            low_end = factor * image
            xb[...] = (factor * (xb[...].astype(f32) + nn(xb[...], rb[...]))).astype(bf16)
            if step < 2:
                rb[...] = (jnp.where(eye, 1.0, 0.0) - nn(s_high[...], xb[...])).astype(bf16)
        residual = jnp.where(eye, 1.0, 0.0) - nn(s_high[...], xb[...]) - nn(s_low[...], xb[...])
        left[...] = residual
        size = jnp.max(jnp.sum(jnp.abs(residual), axis=1, keepdims=True), axis=0, keepdims=True)
        rb[...] = residual.astype(bf16)
        rb[...] = (left[...] + nn(rb[...], rb[...])).astype(bf16)
        rest = nn(xb[...], rb[...])
        h, l = split2(rest)
        eh[...] = h
        el[...] = l

        @pl.when(jnp.logical_not(size[0, 0] < 0.1))
        def _():
            full = functools.partial(jnp.dot, precision=lax.Precision.HIGHEST,
                                     preferred_element_type=f32)
            ident = jnp.where(iota((obs, obs), 0) == iota((obs, obs), 1), 1.0, 0.0)
            rows = jnp.max(jnp.sum(jnp.abs(gram[...]), axis=1, keepdims=True), axis=0, keepdims=True)
            left[...] = ident * (1.0 / rows)

            def advance(carry):
                count, _ = carry
                residual = ident - full(gram[...], left[...])
                error = jnp.sum(residual * residual)
                left[...] = left[...] + full(left[...], residual)
                return count + 1, error

            lax.while_loop(lambda c: (c[0] < 40) & jnp.logical_not(c[1] < 1e-7), advance,
                           (jnp.int32(0), jnp.float32(1.0)))
            xb[...] = left[...].astype(bf16)
            h, l = split2(left[...] - xb[...].astype(f32))
            eh[...] = h
            el[...] = l

        return scale_r, scale_c

    def innovation(b, o_ref, n_ref):
        val_r, var_r = par_ref[4 * b + 1:4 * b + 2, :], par_ref[4 * b + 2:4 * b + 3, :]
        return val_r + jnp.sqrt(var_r) * n_ref[...] - o_ref[...].T

    def weighted_own(b, x):
        pos_c = par_t[:, 4 * b:4 * b + 1]
        xh, xl = split2(x - jnp.mean(x, axis=0, keepdims=True))
        cross = nn(high[...], xh) + nn(high[...], xl) + nn(middle[...], xh)
        return taper(pos_c, pos_dev) * cross * norming

    scale_r, scale_c = invert(0, o0)
    vh, vl = split2(innovation(0, o0, n0) * scale_r)
    solved = nn(vh, xb[...]) + nn(vl, xb[...]) + nn(vh, eh[...]) + nn(vh, el[...])
    sh, sl = split2(solved * scale_r)
    s_high[...] = sh
    s_low[...] = sl
    wh, wl = split2(weighted_own(0, x_ref[...]))
    out_ref[...] = x_ref[...] + nn(s_high[...], wh) + nn(s_high[...], wl) + nn(s_low[...], wh)
    o = o1[...]
    oh, ol = split2(o - jnp.mean(o, axis=1, keepdims=True))
    cross = nt(oh, high[...]) + nt(oh, middle[...]) + nt(ol, high[...])
    wh, wl = split2(taper(par_t[:, 4:5], par_ref[0:1, :]) * cross * norming)
    o1[...] = o1[...] + nt(wh, s_high[...]) + nt(wh, s_low[...]) + nt(wl, s_high[...])
    scale_r, scale_c = invert(1, o1)
    wh, wl = split2(weighted_own(1, out_ref[...]) * scale_c)
    applied = nn(xb[...], wh) + nn(xb[...], wl) + nn(eh[...], wh) + nn(el[...], wh)
    wh, wl = split2(applied * scale_c)
    vh, vl = split2(innovation(1, o1, n1))
    out_ref[...] = out_ref[...] + nn(vh, wh) + nn(vh, wl) + nn(vl, wh)


def ring_gather(value, axis, size):
    parts = [value] + [
        lax.ppermute(value, axis, [(i, (i + k) % size) for i in range(size)])
        for k in range(1, size)
    ]
    return jnp.concatenate(parts, axis=0)


def on_device(state, obs_index, obs_values, obs_var, noise):
    members, rows_dev = state.shape
    batches, obs = obs_index.shape
    cols = lax.axis_size(COL)
    nx, nz, nc = (lax.axis_size(a) for a in ROW)
    nzl, ny = (lax.axis_size(a) for a in COL)
    my_col = lax.axis_index(COL)
    my_tile = lax.axis_index(ROW)
    tile_rows = rows_dev * cols
    bin_rows = tile_rows * nx * nz * nc // POSITIONS
    first = (my_tile * cols + my_col) * rows_dev
    core = lax.axis_index("core")
    slots = cols * batches * SLOTS
    unit = obs // cols // nc
    prep_dims = (tile_rows, bin_rows, cols)

    def scalars(*values):
        return jnp.stack([jnp.asarray(v, i32) for v in values])

    smem = pl.BlockSpec(memory_space=pltpu.SMEM)
    vmem = pl.BlockSpec(memory_space=pltpu.VMEM)

    def call(kernel, shapes, inputs, scratch=(), flops=0):
        return pl.pallas_call(
            kernel,
            out_shape=shapes,
            in_specs=[smem] + [vmem] * (len(inputs) - 1),
            out_specs=jax.tree.map(lambda _: vmem, shapes),
            scratch_shapes=list(scratch),
            cost_estimate=pl.CostEstimate(flops=flops, bytes_accessed=4 << 20, transcendentals=0),
            compiler_params=pltpu.CompilerParams(vmem_limit_bytes=56 << 20),
        )(*inputs)

    send, par, noise_t = call(
        functools.partial(prep_kernel, prep_dims),
        (jax.ShapeDtypeStruct((slots, members), f32),
         jax.ShapeDtypeStruct((4 * batches, obs), f32),
         jax.ShapeDtypeStruct((batches, noise.shape[2], obs), f32)),
        (scalars(my_tile, first, 0), obs_index, obs_values, obs_var, state, noise),
        flops=2 << 30)

    def exchange(send, turn):
        mine = lax.all_to_all(send.reshape(cols, batches * SLOTS, members), COL, 0, 0, tiled=True)
        mine = jnp.sum(mine, axis=0)
        mine = ring_gather(mine, "zh", nz)
        mine = ring_gather(mine, "x", nx)
        mine = ring_gather(mine, "core", nc)
        return call(
            functools.partial(place_kernel, (tile_rows, cols, (nx, nz, nc))),
            jax.ShapeDtypeStruct((batches * unit, members), f32),
            (scalars(my_col, turn, *(lax.axis_index(a) for a in ROW)), obs_index, mine),
            flops=1 << 28)

    held = exchange(send, 0)

    def more(carry):
        turn, held = carry
        send = call(
            functools.partial(send_kernel, prep_dims),
            jax.ShapeDtypeStruct((slots, members), f32),
            (scalars(my_tile, first, turn), obs_index, state))
        return turn + 1, held + exchange(send, turn)

    tiles = obs_index[:, :, None] // tile_rows == jnp.arange(nx * nz * nc, dtype=i32)
    most = jnp.max(jnp.sum(tiles.astype(i32), axis=1))
    turns = (most + cols * SLOTS - 1) // (cols * SLOTS)
    _, held = lax.while_loop(lambda carry: carry[0] < turns, more, (jnp.int32(1), held))

    def everywhere(value):
        value = ring_gather(value, "zl", nzl)
        value = ring_gather(value, "y", ny)
        return value, lax.ppermute(value, "core", [(0, 1), (1, 0)])

    part = noise.shape[2] // nc
    noise_half = lax.dynamic_slice_in_dim(noise_t, core * part, part, axis=1)
    na, nb = everywhere(noise_half.reshape(batches * part, obs))
    o0a, o0b = everywhere(held[:unit])
    o1a, o1b = everywhere(held[unit:])
    full = (obs, members)
    return call(
        functools.partial(main_kernel, (bin_rows, nzl, ny)),
        jax.ShapeDtypeStruct(state.shape, f32),
        (scalars(lax.axis_index("zl"), lax.axis_index("y"), core, first),
         par, o0a, o0b, o1a, o1b, na, nb, state),
        scratch=[pltpu.VMEM(full, f32)] * 6 + [pltpu.VMEM(full, bf16)] * 9,
        flops=20 << 30)


def solution(mesh):
    split = Mesh(mesh.devices.reshape(4, 2, 2, 4, 4), ROW_COL)
    placed = (P(None, ROW_COL), P(), P(), P(), P(None, None, COL))
    return jax.shard_map(
        on_device, mesh=split, in_specs=placed, out_specs=P(None, ROW_COL), check_vma=False
    )
```

```python
import functools

import jax
import jax.numpy as jnp
from jax import lax
from jax.experimental import pallas as pl
from jax.experimental.pallas import tpu as pltpu
from jax.sharding import Mesh
from jax.sharding import PartitionSpec as P


POSITIONS = 256
RADIUS = 64
ROW = ("x", "zh", "core")
COL = ("zl", "y")
ROW_COL = ROW + COL
SLOTS = 4

f32 = jnp.float32
bf16 = jnp.bfloat16
i32 = jnp.int32


def nn(a, b):
    return lax.dot_general(a, b, (((1,), (0,)), ((), ())), preferred_element_type=f32)


def nt(a, b):
    return lax.dot_general(a, b, (((1,), (1,)), ((), ())), preferred_element_type=f32)


def split2(x):
    high = x.astype(bf16)
    return high, (x - high.astype(f32)).astype(bf16)


def split3(x):
    high = x.astype(bf16)
    rest = x - high.astype(f32)
    middle = rest.astype(bf16)
    return high, middle, (rest - middle.astype(f32)).astype(bf16)


def one_hot(mask):
    return jnp.where(mask, 1.0, 0.0).astype(bf16)


def exact_nn(hot, x):
    high, middle, low = split3(x)
    return nn(hot, high) + nn(hot, middle) + nn(hot, low)


def exact_nt(hot, x):
    high, middle, low = split3(x)
    return nt(hot, high) + nt(hot, middle) + nt(hot, low)


def exact_tn(x, hot):
    high, middle, low = split3(x)
    return nt(high, hot) + nt(middle, hot) + nt(low, hot)


def column_of(row):
    return jnp.broadcast_to(row, (128, row.shape[1])).T[:, 0:1]


def iota(shape, dim):
    return lax.broadcasted_iota(i32, shape, dim)


def shift_of(value):
    assert value & (value - 1) == 0
    return value.bit_length() - 1


def right(value, bits):
    return lax.shift_right_logical(value, jnp.full(value.shape, bits, i32))


def order_of(rows, tile_rows, obs):
    tile = right(rows, shift_of(tile_rows))
    key = (tile * obs + iota((1, obs), 1)).astype(f32)
    rank = jnp.sum(jnp.where(column_of(key) < key, 1.0, 0.0), axis=0, keepdims=True)
    rank = rank.astype(i32)
    return tile, rank


def par_kernel(dims, where_ref, index_ref, values_ref, var_ref, noise_ref, par_ref, noise_out_ref):
    bin_rows, tile_rows, cols = dims
    batches, obs = index_ref.shape
    for b in range(batches):
        rows = index_ref[b:b + 1, :]
        _, rank = order_of(rows, tile_rows, obs)
        placed = (rank & (cols - 1)) * (obs // cols) + right(rank, shift_of(cols))
        hot = one_hot(iota((obs, obs), 0) == placed)
        par = jnp.concatenate(
            [right(rows, shift_of(bin_rows)).astype(f32), values_ref[b:b + 1, :],
             var_ref[b:b + 1, :], jnp.zeros((5, obs), f32)], axis=0)
        par_ref[4 * b:4 * b + 4, :] = exact_tn(par, hot)[0:4]
        noise_out_ref[b] = exact_tn(noise_ref[b], hot)


def send_kernel(dims, where_ref, index_ref, state_ref, send_ref):
    tile_rows, _, cols = dims
    _, rows_dev = state_ref.shape
    batches, obs = index_ref.shape
    my_tile, first, turn = where_ref[0], where_ref[1], where_ref[2]
    slots = send_ref.shape[0]
    per_col = slots // cols
    pick = jnp.zeros((slots, rows_dev), f32)
    for b in range(batches):
        rows = index_ref[b:b + 1, :]
        tile, rank = order_of(rows, tile_rows, obs)
        col = rank & (cols - 1)
        start = jnp.sum(jnp.where(tile < my_tile, 1.0, 0.0), axis=1, keepdims=True).astype(i32)
        base = start + ((col - start) & (cols - 1))
        turn_slot = right(rank - base + 16 * cols * obs, shift_of(cols)) - 16 * obs - turn * SLOTS
        local = rows - first
        inside = (local >= 0) & (local < rows_dev) & (turn_slot >= 0) & (turn_slot < SLOTS)
        slot = jnp.where(inside, col * per_col + b * SLOTS + turn_slot, -1)
        pick += nt(one_hot(iota((slots, obs), 0) == slot),
                   one_hot(iota((rows_dev, obs), 0) == local))
    send_ref[...] = exact_nt(pick.astype(bf16), state_ref[...])


def place_kernel(dims, where_ref, index_ref, slots_ref, held_ref, out_ref):
    tile_rows, cols, sizes = dims
    batches, _ = index_ref.shape
    slots = slots_ref.shape[0]
    my_col, turn = where_ref[0], where_ref[1]
    mine = [where_ref[2 + k] for k in range(3)]
    half = out_ref.shape[0] // batches
    p = iota((slots, 1), 0)
    block = right(p, shift_of(batches * SLOTS))
    batch = right(p, shift_of(SLOTS)) & (batches - 1)
    slot = (p & (SLOTS - 1)) + turn * SLOTS
    nx, nz, nc = sizes
    block_z = block & (nz - 1)
    block_x = right(block, shift_of(nz)) & (nx - 1)
    block_c = right(block, shift_of(nz * nx))
    tile_p = (((mine[0] - block_x) & (nx - 1)) * nz + ((mine[1] - block_z) & (nz - 1))) * nc
    tile_p = tile_p + ((mine[2] - block_c) & (nc - 1))
    start = jnp.zeros((slots, 1), i32)
    end = jnp.zeros((slots, 1), i32)
    for b in range(batches):
        tile = right(index_ref[b:b + 1, :], shift_of(tile_rows))
        before = jnp.sum(jnp.where(tile < tile_p, 1.0, 0.0), axis=1, keepdims=True).astype(i32)
        through = jnp.sum(jnp.where(tile <= tile_p, 1.0, 0.0), axis=1, keepdims=True).astype(i32)
        start = jnp.where(batch == b, before, start)
        end = jnp.where(batch == b, through, end)
    rank = start + ((my_col - start) & (cols - 1)) + slot * cols
    j = right(rank - my_col, shift_of(cols)) - mine[2] * half
    target = jnp.where((rank < end) & (j >= 0) & (j < half), batch * half + j, -1)
    wide = 128
    hot = jnp.where(iota((slots, wide), 1) == target, 1.0, 0.0).T.astype(bf16)
    out_ref[...] = held_ref[...] + exact_nn(hot[0:out_ref.shape[0]], slots_ref[...])


def taper(first, second):
    scaled = (first - second) * (1.0 / RADIUS)
    return jnp.exp(-0.5 * scaled * scaled)


def put_in_place(where, source_a, source_b, target, skip, stride, nzl, ny):
    zl, y, core = where
    unit = target.shape[0] // (2 * nzl * ny)
    for source, half in ((source_a, core), (source_b, 1 - core)):
        for dy in range(ny):
            for dz in range(nzl):
                at = ((((zl - dz) & (nzl - 1)) * ny + ((y - dy) & (ny - 1))) * 2 + half) * unit
                k = ((dy * nzl + dz) * stride + skip) * unit
                target[pl.ds(pl.multiple_of(at, unit), unit), :] = source[k:k + unit, :]


def pieces(size, width, body, carry=0):
    def step(k, carry):
        at = k * width
        return body(pl.ds(pl.multiple_of(at, width), width), at, carry)

    return lax.fori_loop(0, size // width, step, carry)


def each(size, width, body):
    def step(ds, at, carry):
        body(ds, at)
        return carry

    pieces(size, width, step)


def eye_part(obs, width, at):
    return iota((obs, width), 0) == iota((obs, width), 1) + at


def ident_part(obs, width, at):
    return jnp.where(eye_part(obs, width, at), 1.0, 0.0)


def centre(o, high, middle, low):
    def rows(ds, at):
        part = o[ds, :]
        part = part - jnp.mean(part, axis=1, keepdims=True)
        high[ds, :], middle[ds, :], low[ds, :] = split3(part)

    each(o.shape[0], 128, rows)


def invert(pos_r, var_r, pos_c, members, high, middle, low, left, gram, other, spare, s_high, s_low,
           xa, xb, ra, rb, eh, el, vec):
    obs = gram.shape[0]
    width = obs // 2
    norming = 1.0 / (members - 1)

    def cross_terms(ds, at):
        left[:, ds] = nt(high[...], middle[ds, :]) + nt(high[...], low[ds, :])

    each(obs, width, cross_terms)

    def covariance(ds, at):
        product = nt(high[...], high[ds, :]) + nt(middle[...], middle[ds, :])
        product = product + left[:, ds] + left[ds, :].T
        eye = eye_part(obs, width, at)
        covar = taper(pos_c, pos_r[:, ds]) * product * norming + jnp.where(eye, var_r[:, ds], 0.0)
        gram[:, ds] = covar
        vec[0:1, ds] = lax.rsqrt(jnp.sum(jnp.where(eye, covar, 0.0), axis=0, keepdims=True))

    each(obs, width, covariance)
    scale_c = column_of(vec[0:1, :])

    def rescale(ds, at):
        scaled = gram[:, ds] * scale_c * vec[0:1, ds]
        gram[:, ds] = scaled
        s_high[:, ds], s_low[:, ds] = split2(scaled)

    each(obs, width, rescale)

    def squared(ds, at):
        square = nn(s_high[...], s_high[:, ds])
        left[:, ds] = square
        vec[1:2, ds] = jnp.sum(jnp.abs(square), axis=0, keepdims=True)

    each(obs, width, squared)
    upper = jnp.sqrt(jnp.max(vec[1:2, :], axis=1, keepdims=True)) * 1.01
    lower = jnp.min(var_r[...] * vec[0:1, :] * vec[0:1, :], axis=1, keepdims=True)
    alpha = 2.0 / (upper + lower)

    def widen(low_end):
        image = low_end * (2.0 - low_end)
        factor = 2.0 / (1.0 + image)
        return factor, factor * image

    factor, low_end = widen(alpha * lower)

    def first(ds, at):
        ident = ident_part(obs, width, at)
        step = alpha * gram[:, ds]
        xa[:, ds] = (factor * alpha * (2.0 * ident - step)).astype(bf16)
        ra[:, ds] = (ident - factor * (2.0 * step - alpha * alpha * left[:, ds])).astype(bf16)

    each(obs, width, first)

    def grow(old, new, factor):
        def part(ds, at):
            new[:, ds] = (factor * (old[:, ds].astype(f32) + nn(old[...], ra[:, ds]))).astype(bf16)

        each(obs, width, part)

    def remain(new):
        def part(ds, at):
            ra[:, ds] = (ident_part(obs, width, at) - nn(s_high[...], new[:, ds])).astype(bf16)

        each(obs, width, part)

    factor, low_end = widen(low_end)
    grow(xa, xb, factor)
    remain(xb)
    factor, low_end = widen(low_end)
    grow(xb, xa, factor)
    remain(xa)
    factor, low_end = widen(low_end)
    grow(xa, xb, factor)

    def remain_last(ds, at):
        residual = (ident_part(obs, width, at)
                    - nn(s_high[...], xb[:, ds]) - nn(s_low[...], xb[:, ds]))
        left[:, ds] = residual
        ra[:, ds] = residual.astype(bf16)
        vec[1:2, ds] = jnp.sum(jnp.abs(residual), axis=0, keepdims=True)

    each(obs, width, remain_last)

    def second_order(ds, at):
        rb[:, ds] = (left[:, ds] + nn(ra[...], ra[:, ds])).astype(bf16)

    each(obs, width, second_order)

    def correction(ds, at):
        eh[:, ds], el[:, ds] = split2(nn(xb[...], rb[:, ds]))

    each(obs, width, correction)
    size = jnp.max(vec[1:2, :], axis=1, keepdims=True)

    @pl.when(jnp.logical_not(size[0, 0] < 0.1))
    def _():
        narrow = 128
        full = functools.partial(jnp.dot, precision=lax.Precision.HIGHEST,
                                 preferred_element_type=f32)
        sums = jnp.sum(jnp.abs(gram[...]), axis=0, keepdims=True)
        guess = 1.0 / jnp.max(sums, axis=1, keepdims=True)

        def start(ds, at):
            left[:, ds] = ident_part(obs, narrow, at) * guess

        each(obs, narrow, start)

        def blocks(body, carry):
            def across(ds, at, carry):
                return pieces(obs, narrow, lambda dr, ar, c: body(dr, ar, ds, at, c), carry)

            return pieces(obs, narrow, across, carry)

        def advance(carry):
            def residuals(dr, ar, ds, at, error):
                eye = iota((narrow, narrow), 0) + ar == iota((narrow, narrow), 1) + at
                residual = jnp.where(eye, 1.0, 0.0) - full(gram[dr, :], left[:, ds])
                other[dr, ds] = residual
                return error + jnp.sum(residual * residual)

            def update(dr, ar, ds, at, carry):
                spare[dr, ds] = left[dr, ds] + full(left[dr, :], other[:, ds])
                return carry

            error = blocks(residuals, jnp.float32(0.0))
            blocks(update, 0)
            left[...] = spare[...]
            return carry[0] + 1, error

        lax.while_loop(lambda c: (c[0] < 40) & jnp.logical_not(c[1] < 1e-7), advance,
                       (jnp.int32(0), jnp.float32(1.0)))
        xb[...] = left[...].astype(bf16)
        eh[...], el[...] = split2(left[...] - xb[...].astype(f32))


def innovate(val_r, var_r, scale_r, o, n, vh, vl):
    deviation = jnp.sqrt(var_r)

    def rows(ds, at):
        part = val_r + deviation * n[ds, :] - o[:, ds].T
        vh[ds, :], vl[ds, :] = split2(part * scale_r)

    each(n.shape[0], 128, rows)


def weigh(pos_c, pos_dev, x, high, middle, members):
    xh, xl = split2(x - jnp.mean(x, axis=0, keepdims=True))
    cross = nn(high[...], xh) + nn(high[...], xl) + nn(middle[...], xh)
    return taper(pos_c, pos_dev) * cross * (1.0 / (members - 1))


def columns(par_ref):
    return jnp.concatenate([par_ref[...], jnp.zeros((120, par_ref.shape[1]), f32)], axis=0).T


def own_positions(first, rows_dev, bin_rows):
    return right(first + iota((1, rows_dev), 1), shift_of(bin_rows)).astype(f32)


def first_kernel(dims, where_ref, par_ref, oa, ob, x_ref,
                 o, high, middle, xb, eh, el, vec, wh, wl, *work):
    bin_rows, nzl, ny = dims
    where = [where_ref[k] for k in range(3)]
    _, members = o.shape
    low, left, gram, other, spare, s_high, s_low, xa, ra, rb = work
    put_in_place(where, oa, ob, o, 0, 1, nzl, ny)
    pos_c = columns(par_ref)[:, 0:1]
    pos_dev = own_positions(where_ref[3], x_ref.shape[1], bin_rows)
    centre(o, high, middle, low)
    invert(par_ref.at[0:1], par_ref.at[2:3], pos_c, members, high, middle, low, left, gram, other,
           spare, s_high, s_low, xa, xb, ra, rb, eh, el, vec)
    wh[...], wl[...] = split2(weigh(pos_c, pos_dev, x_ref[...], high, middle, members))


def second_kernel(dims, where_ref, par_ref, oa, ob, na, nb, x_ref,
                  o0, high0, middle0, xb0, eh0, el0, vec0, wh0, wl0,
                  out_ref, high, middle, o, n, vh, vl, sh, sl, xb, eh, el, vec, *work):
    bin_rows, nzl, ny = dims
    where = [where_ref[k] for k in range(3)]
    obs, members = o.shape
    low, left, gram, other, spare, s_high, s_low, xa, ra, rb = work
    pos_c = columns(par_ref)[:, 4:5]
    pos_dev = own_positions(where_ref[3], x_ref.shape[1], bin_rows)
    norming = 1.0 / (members - 1)
    put_in_place(where, na, nb, n, 0, 2, nzl, ny)
    innovate(par_ref[1:2, :], par_ref[2:3, :], vec0[0:1, :], o0, n, vh, vl)

    def solve(ds, at):
        part = nn(vh[...], xb0[:, ds]) + nn(vl[...], xb0[:, ds])
        part = part + nn(vh[...], eh0[:, ds]) + nn(vh[...], el0[:, ds])
        sh[:, ds], sl[:, ds] = split2(part * vec0[0:1, ds])

    each(obs, obs // 2, solve)
    out_ref[...] = (x_ref[...] + nn(sh[...], wh0[...]) + nn(sh[...], wl0[...])
                    + nn(sl[...], wh0[...]))
    put_in_place(where, oa, ob, o, 0, 1, nzl, ny)
    put_in_place(where, na, nb, n, 1, 2, nzl, ny)
    centre(o, high, middle, low)

    def weights(ds, at):
        cross = nt(high[...], high0[ds, :]) + nt(high[...], middle0[ds, :])
        cross = cross + nt(middle[...], high0[ds, :])
        xa[:, ds], xb[:, ds] = split2(taper(pos_c, par_ref[0:1, ds]) * cross * norming)

    each(obs, obs // 2, weights)

    def update(ds, at):
        o[:, ds] = (o[:, ds] + nt(xa[...], sh[ds, :]) + nt(xa[...], sl[ds, :])
                    + nt(xb[...], sh[ds, :]))

    each(members, members // 2, update)
    centre(o, high, middle, low)
    invert(par_ref.at[4:5], par_ref.at[6:7], pos_c, members, high, middle, low, left, gram, other,
           spare, s_high, s_low, xa, xb, ra, rb, eh, el, vec)
    scale_c = column_of(vec[0:1, :])
    wh, wl = split2(weigh(pos_c, pos_dev, out_ref[...], high, middle, members) * scale_c)
    applied = nn(xb[...], wh) + nn(xb[...], wl) + nn(eh[...], wh) + nn(el[...], wh)
    wh, wl = split2(applied * scale_c)
    innovate(par_ref[5:6, :], par_ref[6:7, :], jnp.ones((1, obs), f32), o, n, vh, vl)
    out_ref[...] = out_ref[...] + nn(vh[...], wh) + nn(vh[...], wl) + nn(vl[...], wh)


def ring_gather(value, axis, size):
    parts = [value] + [
        lax.ppermute(value, axis, [(i, (i + k) % size) for i in range(size)])
        for k in range(1, size)
    ]
    return jnp.concatenate(parts, axis=0)


def on_device(state, obs_index, obs_values, obs_var, noise):
    members, rows_dev = state.shape
    batches, obs = obs_index.shape
    cols = lax.axis_size(COL)
    nx, nz, nc = (lax.axis_size(a) for a in ROW)
    nzl, ny = (lax.axis_size(a) for a in COL)
    my_col = lax.axis_index(COL)
    my_tile = lax.axis_index(ROW)
    tile_rows = rows_dev * cols
    bin_rows = tile_rows * nx * nz * nc // POSITIONS
    first = (my_tile * cols + my_col) * rows_dev
    core = lax.axis_index("core")
    noise = jnp.swapaxes(noise, 1, 2)
    slots = cols * batches * SLOTS
    unit = obs // cols // nc
    prep_dims = (tile_rows, bin_rows, cols)

    def scalars(*values):
        return jnp.stack([jnp.asarray(v, i32) for v in values])

    smem = pl.BlockSpec(memory_space=pltpu.SMEM)
    vmem = pl.BlockSpec(memory_space=pltpu.VMEM)

    def call(kernel, shapes, inputs, scratch=(), flops=0, room=16):
        return pl.pallas_call(
            kernel,
            out_shape=shapes,
            in_specs=[smem] + [vmem] * (len(inputs) - 1),
            out_specs=jax.tree.map(lambda _: vmem, shapes),
            scratch_shapes=list(scratch),
            cost_estimate=pl.CostEstimate(flops=flops, bytes_accessed=4 << 20, transcendentals=0),
            compiler_params=pltpu.CompilerParams(vmem_limit_bytes=room << 20),
        )(*inputs)

    par, noise_t = call(
        functools.partial(par_kernel, (bin_rows, tile_rows, cols)),
        (jax.ShapeDtypeStruct((4 * batches, obs), f32), jax.ShapeDtypeStruct(noise.shape, f32)),
        (scalars(0), obs_index, obs_values, obs_var, noise), flops=1 << 30)

    def exchange(turn, held):
        send = call(
            functools.partial(send_kernel, prep_dims),
            jax.ShapeDtypeStruct((slots, members), f32),
            (scalars(my_tile, first, turn), obs_index, state), flops=1 << 28)
        mine = lax.all_to_all(send.reshape(cols, batches * SLOTS, members), COL, 0, 0, tiled=True)
        mine = jnp.sum(mine, axis=0)
        mine = ring_gather(mine, "zh", nz)
        mine = ring_gather(mine, "x", nx)
        mine = ring_gather(mine, "core", nc)
        return call(
            functools.partial(place_kernel, (tile_rows, cols, (nx, nz, nc))),
            jax.ShapeDtypeStruct((batches * unit, members), f32),
            (scalars(my_col, turn, *(lax.axis_index(a) for a in ROW)), obs_index, mine, held),
            flops=1 << 28)

    tiles = obs_index[:, :, None] // tile_rows == jnp.arange(nx * nz * nc, dtype=i32)
    most = jnp.max(jnp.sum(tiles.astype(i32), axis=1))
    turns = (most + cols * SLOTS - 1) // (cols * SLOTS)
    held = lax.fori_loop(0, turns, exchange, jnp.zeros((batches * unit, members), f32))

    swap = [(0, 1), (1, 0)]
    part = noise.shape[1] // nc
    noise_half = lax.dynamic_slice_in_dim(noise_t, core * part, part, axis=1)
    na = ring_gather(noise_half.reshape(batches * part, obs), "zl", nzl)
    na, held = lax.optimization_barrier((na, held))
    na = ring_gather(na, "y", ny)
    oa, later = held[:unit], held[unit:]
    oa = ring_gather(oa, "zl", nzl)
    oa, later = lax.optimization_barrier((oa, later))
    oa = ring_gather(oa, "y", ny)
    ob = lax.ppermute(oa, "core", swap)
    la = ring_gather(later, "zl", nzl)
    la = ring_gather(la, "y", ny)
    full = (obs, members)
    wide, slim = pltpu.VMEM(full, f32), pltpu.VMEM(full, bf16)
    work = [slim] + [wide] * 4 + [slim] * 5
    where = scalars(lax.axis_index("zl"), lax.axis_index("y"), core, first)
    dims = (bin_rows, nzl, ny)
    halved = jax.ShapeDtypeStruct(full, bf16)
    weights = jax.ShapeDtypeStruct((obs, rows_dev), bf16)
    found = call(
        functools.partial(first_kernel, dims),
        (jax.ShapeDtypeStruct(full, f32), halved, halved, halved, halved, halved,
         jax.ShapeDtypeStruct((8, obs), f32), weights, weights),
        (where, par, oa, ob, state), scratch=work, flops=7 << 30, room=24)
    la, na, *found = lax.optimization_barrier((la, na, *found))
    lb = lax.ppermute(la, "core", swap)
    nb = lax.ppermute(na, "core", swap)
    return call(
        functools.partial(second_kernel, dims),
        jax.ShapeDtypeStruct(state.shape, f32),
        (where, par, la, lb, na, nb, state, *found),
        scratch=([slim] * 2 + [wide] * 2 + [slim] * 7 + [pltpu.VMEM((8, obs), f32)] + work),
        flops=12 << 30, room=30)


def solution(mesh):
    split = Mesh(mesh.devices.reshape(4, 2, 2, 4, 4), ROW_COL)
    placed = (P(None, ROW_COL), P(), P(), P(), P(None, None, COL))

    return jax.shard_map(
        on_device, mesh=split, in_specs=placed, out_specs=P(None, ROW_COL), check_vma=False
    )
```

```python
import functools

import jax
import jax.numpy as jnp
from jax import lax
from jax.experimental import pallas as pl
from jax.experimental.pallas import tpu as pltpu
from jax.sharding import Mesh
from jax.sharding import PartitionSpec as P


POSITIONS = 256
RADIUS = 64
ROW = ("x", "zh", "core")
COL = ("zl", "y")
ROW_COL = ROW + COL
SLOTS = 4

f32 = jnp.float32
bf16 = jnp.bfloat16
i32 = jnp.int32


def nn(a, b):
    return lax.dot_general(a, b, (((1,), (0,)), ((), ())), preferred_element_type=f32)


def nt(a, b):
    return lax.dot_general(a, b, (((1,), (1,)), ((), ())), preferred_element_type=f32)


def split2(x):
    high = x.astype(bf16)
    return high, (x - high.astype(f32)).astype(bf16)


def split3(x):
    high = x.astype(bf16)
    rest = x - high.astype(f32)
    middle = rest.astype(bf16)
    return high, middle, (rest - middle.astype(f32)).astype(bf16)


def one_hot(mask):
    return jnp.where(mask, 1.0, 0.0).astype(bf16)


def exact_nn(hot, x):
    high, middle, low = split3(x)
    return nn(hot, high) + nn(hot, middle) + nn(hot, low)


def exact_nt(hot, x):
    high, middle, low = split3(x)
    return nt(hot, high) + nt(hot, middle) + nt(hot, low)


def exact_tn(x, hot):
    high, middle, low = split3(x)
    return nt(high, hot) + nt(middle, hot) + nt(low, hot)


def column_of(row):
    return jnp.broadcast_to(row, (128, row.shape[1])).T[:, 0:1]


def iota(shape, dim):
    return lax.broadcasted_iota(i32, shape, dim)


def shift_of(value):
    assert value & (value - 1) == 0
    return value.bit_length() - 1


def right(value, bits):
    return lax.shift_right_logical(value, jnp.full(value.shape, bits, i32))


def order_of(rows, tile_rows, obs):
    tile = right(rows, shift_of(tile_rows))
    key = (tile * obs + iota((1, obs), 1)).astype(f32)
    rank = jnp.sum(jnp.where(column_of(key) < key, 1.0, 0.0), axis=0, keepdims=True)
    rank = rank.astype(i32)
    return tile, rank


def par_kernel(dims, where_ref, index_ref, values_ref, var_ref, noise_ref, par_ref, noise_out_ref):
    bin_rows, tile_rows, cols = dims
    batches, obs = index_ref.shape
    for b in range(batches):
        rows = index_ref[b:b + 1, :]
        _, rank = order_of(rows, tile_rows, obs)
        placed = (rank & (cols - 1)) * (obs // cols) + right(rank, shift_of(cols))
        hot = one_hot(iota((obs, obs), 0) == placed)
        par = jnp.concatenate(
            [right(rows, shift_of(bin_rows)).astype(f32), values_ref[b:b + 1, :],
             var_ref[b:b + 1, :], jnp.zeros((5, obs), f32)], axis=0)
        par_ref[4 * b:4 * b + 4, :] = exact_tn(par, hot)[0:4]
        noise_out_ref[b] = exact_tn(noise_ref[b], hot)


def send_kernel(dims, where_ref, index_ref, state_ref, send_ref):
    tile_rows, _, cols = dims
    _, rows_dev = state_ref.shape
    batches, obs = index_ref.shape
    my_tile, first, turn = where_ref[0], where_ref[1], where_ref[2]
    slots = send_ref.shape[0]
    per_col = slots // cols
    pick = jnp.zeros((slots, rows_dev), f32)
    for b in range(batches):
        rows = index_ref[b:b + 1, :]
        tile, rank = order_of(rows, tile_rows, obs)
        col = rank & (cols - 1)
        start = jnp.sum(jnp.where(tile < my_tile, 1.0, 0.0), axis=1, keepdims=True).astype(i32)
        base = start + ((col - start) & (cols - 1))
        turn_slot = right(rank - base + 16 * cols * obs, shift_of(cols)) - 16 * obs - turn * SLOTS
        local = rows - first
        inside = (local >= 0) & (local < rows_dev) & (turn_slot >= 0) & (turn_slot < SLOTS)
        slot = jnp.where(inside, col * per_col + b * SLOTS + turn_slot, -1)
        pick += nt(one_hot(iota((slots, obs), 0) == slot),
                   one_hot(iota((rows_dev, obs), 0) == local))
    send_ref[...] = exact_nt(pick.astype(bf16), state_ref[...])


def place_kernel(dims, where_ref, index_ref, slots_ref, held_ref, out_ref):
    tile_rows, cols, sizes = dims
    batches, _ = index_ref.shape
    slots = slots_ref.shape[0]
    my_col, turn = where_ref[0], where_ref[1]
    mine = [where_ref[2 + k] for k in range(3)]
    half = out_ref.shape[0] // batches
    p = iota((slots, 1), 0)
    block = right(p, shift_of(batches * SLOTS))
    batch = right(p, shift_of(SLOTS)) & (batches - 1)
    slot = (p & (SLOTS - 1)) + turn * SLOTS
    nx, nz, nc = sizes
    block_z = block & (nz - 1)
    block_x = right(block, shift_of(nz)) & (nx - 1)
    block_c = right(block, shift_of(nz * nx))
    tile_p = (((mine[0] - block_x) & (nx - 1)) * nz + ((mine[1] - block_z) & (nz - 1))) * nc
    tile_p = tile_p + ((mine[2] - block_c) & (nc - 1))
    start = jnp.zeros((slots, 1), i32)
    end = jnp.zeros((slots, 1), i32)
    for b in range(batches):
        tile = right(index_ref[b:b + 1, :], shift_of(tile_rows))
        before = jnp.sum(jnp.where(tile < tile_p, 1.0, 0.0), axis=1, keepdims=True).astype(i32)
        through = jnp.sum(jnp.where(tile <= tile_p, 1.0, 0.0), axis=1, keepdims=True).astype(i32)
        start = jnp.where(batch == b, before, start)
        end = jnp.where(batch == b, through, end)
    rank = start + ((my_col - start) & (cols - 1)) + slot * cols
    j = right(rank - my_col, shift_of(cols)) - mine[2] * half
    target = jnp.where((rank < end) & (j >= 0) & (j < half), batch * half + j, -1)
    wide = 128
    hot = jnp.where(iota((slots, wide), 1) == target, 1.0, 0.0).T.astype(bf16)
    out_ref[...] = held_ref[...] + exact_nn(hot[0:out_ref.shape[0]], slots_ref[...])


def taper(first, second):
    scaled = (first - second) * (1.0 / RADIUS)
    return jnp.exp(-0.5 * scaled * scaled)


def put_in_place(where, source_a, source_b, target, skip, stride, nzl, ny):
    zl, y, core = where
    unit = target.shape[0] // (2 * nzl * ny)
    for source, half in ((source_a, core), (source_b, 1 - core)):
        for dy in range(ny):
            for dz in range(nzl):
                at = ((((zl - dz) & (nzl - 1)) * ny + ((y - dy) & (ny - 1))) * 2 + half) * unit
                k = ((dy * nzl + dz) * stride + skip) * unit
                target[pl.ds(pl.multiple_of(at, unit), unit), :] = source[k:k + unit, :]


def pieces(size, width, body, carry=0):
    def step(k, carry):
        at = k * width
        return body(pl.ds(pl.multiple_of(at, width), width), at, carry)

    return lax.fori_loop(0, size // width, step, carry)


def each(size, width, body):
    for at in range(0, size, width):
        body(slice(at, at + width), at)


def eye_part(obs, width, at):
    return iota((obs, width), 0) == iota((obs, width), 1) + at


def ident_part(obs, width, at):
    return jnp.where(eye_part(obs, width, at), 1.0, 0.0)


def centre(o, high, middle, low):
    def rows(ds, at):
        part = o[ds, :]
        part = part - jnp.mean(part, axis=1, keepdims=True)
        high[ds, :], middle[ds, :], low[ds, :] = split3(part)

    each(o.shape[0], 128, rows)


def invert(pos_r, var_r, pos_c, members, high, middle, low, left, gram, other, spare, s_high, s_low,
           xa, xb, ra, rb, eh, el, vec):
    obs = gram.shape[0]
    width = obs
    norming = 1.0 / (members - 1)

    def cross_terms(ds, at):
        left[:, ds] = nt(high[...], middle[ds, :]) + nt(high[...], low[ds, :])

    each(obs, width, cross_terms)

    def covariance(ds, at):
        product = nt(high[...], high[ds, :]) + nt(middle[...], middle[ds, :])
        product = product + left[:, ds] + left[ds, :].T
        eye = eye_part(obs, width, at)
        covar = taper(pos_c, pos_r[:, ds]) * product * norming + jnp.where(eye, var_r[:, ds], 0.0)
        gram[:, ds] = covar
        vec[0:1, ds] = lax.rsqrt(jnp.sum(jnp.where(eye, covar, 0.0), axis=0, keepdims=True))

    each(obs, width, covariance)
    scale_c = column_of(vec[0:1, :])

    def rescale(ds, at):
        scaled = gram[:, ds] * scale_c * vec[0:1, ds]
        gram[:, ds] = scaled
        s_high[:, ds], s_low[:, ds] = split2(scaled)

    each(obs, width, rescale)

    def squared(ds, at):
        square = nn(s_high[...], s_high[:, ds])
        left[:, ds] = square
        vec[1:2, ds] = jnp.sum(jnp.abs(square), axis=0, keepdims=True)

    each(obs, width, squared)
    upper = jnp.sqrt(jnp.max(vec[1:2, :], axis=1, keepdims=True)) * 1.01
    lower = jnp.min(var_r[...] * vec[0:1, :] * vec[0:1, :], axis=1, keepdims=True)
    alpha = 2.0 / (upper + lower)

    def widen(low_end):
        image = low_end * (2.0 - low_end)
        factor = 2.0 / (1.0 + image)
        return factor, factor * image

    factor, low_end = widen(alpha * lower)

    def first(ds, at):
        ident = ident_part(obs, width, at)
        step = alpha * gram[:, ds]
        xa[:, ds] = (factor * alpha * (2.0 * ident - step)).astype(bf16)
        ra[:, ds] = (ident - factor * (2.0 * step - alpha * alpha * left[:, ds])).astype(bf16)

    each(obs, width, first)

    def grow(old, new, factor):
        def part(ds, at):
            new[:, ds] = (factor * (old[:, ds].astype(f32) + nn(old[...], ra[:, ds]))).astype(bf16)

        each(obs, width, part)

    def remain(new):
        def part(ds, at):
            ra[:, ds] = (ident_part(obs, width, at) - nn(s_high[...], new[:, ds])).astype(bf16)

        each(obs, width, part)

    factor, low_end = widen(low_end)
    grow(xa, xb, factor)
    remain(xb)
    factor, low_end = widen(low_end)
    grow(xb, xa, factor)
    remain(xa)
    factor, low_end = widen(low_end)
    grow(xa, xb, factor)

    def remain_last(ds, at):
        residual = (ident_part(obs, width, at)
                    - nn(s_high[...], xb[:, ds]) - nn(s_low[...], xb[:, ds]))
        left[:, ds] = residual
        ra[:, ds] = residual.astype(bf16)
        vec[1:2, ds] = jnp.sum(jnp.abs(residual), axis=0, keepdims=True)

    each(obs, width, remain_last)

    def second_order(ds, at):
        rb[:, ds] = (left[:, ds] + nn(ra[...], ra[:, ds])).astype(bf16)

    each(obs, width, second_order)

    def correction(ds, at):
        eh[:, ds], el[:, ds] = split2(nn(xb[...], rb[:, ds]))

    each(obs, width, correction)
    size = jnp.max(vec[1:2, :], axis=1, keepdims=True)

    @pl.when(jnp.logical_not(size[0, 0] < 0.1))
    def _():
        narrow = 128
        full = functools.partial(jnp.dot, precision=lax.Precision.HIGHEST,
                                 preferred_element_type=f32)
        sums = jnp.sum(jnp.abs(gram[...]), axis=0, keepdims=True)
        guess = 1.0 / jnp.max(sums, axis=1, keepdims=True)

        def start(ds, at):
            left[:, ds] = ident_part(obs, narrow, at) * guess

        each(obs, narrow, start)

        def blocks(body, carry):
            def across(ds, at, carry):
                return pieces(obs, narrow, lambda dr, ar, c: body(dr, ar, ds, at, c), carry)

            return pieces(obs, narrow, across, carry)

        def advance(carry):
            def residuals(dr, ar, ds, at, error):
                eye = iota((narrow, narrow), 0) + ar == iota((narrow, narrow), 1) + at
                residual = jnp.where(eye, 1.0, 0.0) - full(gram[dr, :], left[:, ds])
                other[dr, ds] = residual
                return error + jnp.sum(residual * residual)

            def update(dr, ar, ds, at, carry):
                spare[dr, ds] = left[dr, ds] + full(left[dr, :], other[:, ds])
                return carry

            error = blocks(residuals, jnp.float32(0.0))
            blocks(update, 0)
            left[...] = spare[...]
            return carry[0] + 1, error

        lax.while_loop(lambda c: (c[0] < 40) & jnp.logical_not(c[1] < 1e-7), advance,
                       (jnp.int32(0), jnp.float32(1.0)))
        xb[...] = left[...].astype(bf16)
        eh[...], el[...] = split2(left[...] - xb[...].astype(f32))


def innovate(val_r, var_r, scale_r, o, n, vh, vl):
    deviation = jnp.sqrt(var_r)

    def rows(ds, at):
        part = val_r + deviation * n[ds, :] - o[:, ds].T
        vh[ds, :], vl[ds, :] = split2(part * scale_r)

    each(n.shape[0], 128, rows)


def weigh(pos_c, pos_dev, x, high, middle, members):
    xh, xl = split2(x - jnp.mean(x, axis=0, keepdims=True))
    cross = nn(high[...], xh) + nn(high[...], xl) + nn(middle[...], xh)
    return taper(pos_c, pos_dev) * cross * (1.0 / (members - 1))


def columns(par_ref):
    return jnp.concatenate([par_ref[...], jnp.zeros((120, par_ref.shape[1]), f32)], axis=0).T


def own_positions(first, rows_dev, bin_rows):
    return right(first + iota((1, rows_dev), 1), shift_of(bin_rows)).astype(f32)


def main_kernel(dims, where_ref, par_ref, oa, ob, na, nb, x_ref, out_ref,
                high0, middle0, high, middle, o0, o, n, vh, vl, sh, sl, xb, eh, el, vec, *work):
    bin_rows, nzl, ny = dims
    where = [where_ref[k] for k in range(3)]
    obs, members = o.shape
    low, left, gram, other, spare, s_high, s_low, xa, ra, rb = work
    cols_par = columns(par_ref)
    pos_dev = own_positions(where_ref[3], x_ref.shape[1], bin_rows)
    norming = 1.0 / (members - 1)
    put_in_place(where, oa, ob, o0, 0, 2, nzl, ny)
    put_in_place(where, na, nb, n, 0, 2, nzl, ny)
    pos_c = cols_par[:, 0:1]
    centre(o0, high0, middle0, low)
    invert(par_ref.at[0:1], par_ref.at[2:3], pos_c, members, high0, middle0, low, left, gram,
           other, spare, s_high, s_low, xa, xb, ra, rb, eh, el, vec)
    innovate(par_ref[1:2, :], par_ref[2:3, :], vec[0:1, :], o0, n, vh, vl)
    solved = nn(vh[...], xb[...]) + nn(vl[...], xb[...]) + nn(vh[...], eh[...])
    solved = solved + nn(vh[...], el[...])
    sh[...], sl[...] = split2(solved * vec[0:1, :])
    wh, wl = split2(weigh(pos_c, pos_dev, x_ref[...], high0, middle0, members))
    out_ref[...] = x_ref[...] + nn(sh[...], wh) + nn(sh[...], wl) + nn(sl[...], wh)
    put_in_place(where, oa, ob, o, 1, 2, nzl, ny)
    put_in_place(where, na, nb, n, 1, 2, nzl, ny)
    pos_c = cols_par[:, 4:5]
    centre(o, high, middle, low)

    def weights(ds, at):
        cross = nt(high[...], high0[ds, :]) + nt(high[...], middle0[ds, :])
        cross = cross + nt(middle[...], high0[ds, :])
        xa[:, ds], xb[:, ds] = split2(taper(pos_c, par_ref[0:1, ds]) * cross * norming)

    each(obs, obs, weights)

    def update(ds, at):
        o[:, ds] = (o[:, ds] + nt(xa[...], sh[ds, :]) + nt(xa[...], sl[ds, :])
                    + nt(xb[...], sh[ds, :]))

    each(members, members, update)
    centre(o, high, middle, low)
    invert(par_ref.at[4:5], par_ref.at[6:7], pos_c, members, high, middle, low, left, gram, other,
           spare, s_high, s_low, xa, xb, ra, rb, eh, el, vec)
    scale_c = column_of(vec[0:1, :])
    wh, wl = split2(weigh(pos_c, pos_dev, out_ref[...], high, middle, members) * scale_c)
    applied = nn(xb[...], wh) + nn(xb[...], wl) + nn(eh[...], wh) + nn(el[...], wh)
    wh, wl = split2(applied * scale_c)
    innovate(par_ref[5:6, :], par_ref[6:7, :], jnp.ones((1, obs), f32), o, n, vh, vl)
    out_ref[...] = out_ref[...] + nn(vh[...], wh) + nn(vh[...], wl) + nn(vl[...], wh)


def ring_gather(value, axis, size):
    parts = [value] + [
        lax.ppermute(value, axis, [(i, (i + k) % size) for i in range(size)])
        for k in range(1, size)
    ]
    return jnp.concatenate(parts, axis=0)


def on_device(state, obs_index, obs_values, obs_var, noise):
    members, rows_dev = state.shape
    batches, obs = obs_index.shape
    cols = lax.axis_size(COL)
    nx, nz, nc = (lax.axis_size(a) for a in ROW)
    nzl, ny = (lax.axis_size(a) for a in COL)
    my_col = lax.axis_index(COL)
    my_tile = lax.axis_index(ROW)
    tile_rows = rows_dev * cols
    bin_rows = tile_rows * nx * nz * nc // POSITIONS
    first = (my_tile * cols + my_col) * rows_dev
    core = lax.axis_index("core")
    noise = jnp.swapaxes(noise, 1, 2)
    slots = cols * batches * SLOTS
    unit = obs // cols // nc
    prep_dims = (tile_rows, bin_rows, cols)

    def scalars(*values):
        return jnp.stack([jnp.asarray(v, i32) for v in values])

    smem = pl.BlockSpec(memory_space=pltpu.SMEM)
    vmem = pl.BlockSpec(memory_space=pltpu.VMEM)

    def call(kernel, shapes, inputs, scratch=(), flops=0, room=16):
        return pl.pallas_call(
            kernel,
            out_shape=shapes,
            in_specs=[smem] + [vmem] * (len(inputs) - 1),
            out_specs=jax.tree.map(lambda _: vmem, shapes),
            scratch_shapes=list(scratch),
            cost_estimate=pl.CostEstimate(flops=flops, bytes_accessed=4 << 20, transcendentals=0),
            compiler_params=pltpu.CompilerParams(vmem_limit_bytes=room << 20),
        )(*inputs)

    par, noise_t = call(
        functools.partial(par_kernel, (bin_rows, tile_rows, cols)),
        (jax.ShapeDtypeStruct((4 * batches, obs), f32), jax.ShapeDtypeStruct(noise.shape, f32)),
        (scalars(0), obs_index, obs_values, obs_var, noise), flops=1 << 30)

    def exchange(turn, held):
        send = call(
            functools.partial(send_kernel, prep_dims),
            jax.ShapeDtypeStruct((slots, members), f32),
            (scalars(my_tile, first, turn), obs_index, state), flops=1 << 28)
        mine = lax.all_to_all(send.reshape(cols, batches * SLOTS, members), COL, 0, 0, tiled=True)
        mine = jnp.sum(mine, axis=0)
        mine = ring_gather(mine, "zh", nz)
        mine = ring_gather(mine, "x", nx)
        mine = ring_gather(mine, "core", nc)
        return call(
            functools.partial(place_kernel, (tile_rows, cols, (nx, nz, nc))),
            jax.ShapeDtypeStruct((batches * unit, members), f32),
            (scalars(my_col, turn, *(lax.axis_index(a) for a in ROW)), obs_index, mine, held),
            flops=1 << 28)

    tiles = obs_index[:, :, None] // tile_rows == jnp.arange(nx * nz * nc, dtype=i32)
    most = jnp.max(jnp.sum(tiles.astype(i32), axis=1))
    turns = (most + cols * SLOTS - 1) // (cols * SLOTS)
    held = lax.fori_loop(0, turns, exchange, jnp.zeros((batches * unit, members), f32))

    swap = [(0, 1), (1, 0)]
    part = noise.shape[1] // nc
    noise_half = lax.dynamic_slice_in_dim(noise_t, core * part, part, axis=1)
    na = ring_gather(noise_half.reshape(batches * part, obs), "zl", nzl)
    na, held = lax.optimization_barrier((na, held))
    na = ring_gather(na, "y", ny)
    oa = ring_gather(held, "zl", nzl)
    oa = ring_gather(oa, "y", ny)
    ob = lax.ppermute(oa, "core", swap)
    nb = lax.ppermute(na, "core", swap)
    full = (obs, members)
    wide, slim = pltpu.VMEM(full, f32), pltpu.VMEM(full, bf16)
    where = scalars(lax.axis_index("zl"), lax.axis_index("y"), core, first)
    return call(
        functools.partial(main_kernel, (bin_rows, nzl, ny)),
        jax.ShapeDtypeStruct(state.shape, f32),
        (where, par, oa, ob, na, nb, state),
        scratch=([slim] * 4 + [wide] * 3 + [slim] * 7 + [pltpu.VMEM((8, obs), f32)]
                 + [slim] + [wide] * 4 + [slim] * 5),
        flops=20 << 30, room=32)


def solution(mesh):
    split = Mesh(mesh.devices.reshape(4, 2, 2, 4, 4), ROW_COL)
    placed = (P(None, ROW_COL), P(), P(), P(), P(None, None, COL))

    return jax.shard_map(
        on_device, mesh=split, in_specs=placed, out_specs=P(None, ROW_COL), check_vma=False
    )
```

```python
import functools

import jax
import jax.numpy as jnp
from jax import lax
from jax.experimental import pallas as pl
from jax.experimental.pallas import tpu as pltpu
from jax.sharding import Mesh
from jax.sharding import PartitionSpec as P


POSITIONS = 256
RADIUS = 64
ROW = ("x", "zh", "core")
COL = ("zl", "y")
ROW_COL = ROW + COL
SLOTS = 4

f32 = jnp.float32
bf16 = jnp.bfloat16
i32 = jnp.int32


def nn(a, b):
    return lax.dot_general(a, b, (((1,), (0,)), ((), ())), preferred_element_type=f32)


def nt(a, b):
    return lax.dot_general(a, b, (((1,), (1,)), ((), ())), preferred_element_type=f32)


def split2(x):
    high = x.astype(bf16)
    return high, (x - high.astype(f32)).astype(bf16)


def split3(x):
    high = x.astype(bf16)
    rest = x - high.astype(f32)
    middle = rest.astype(bf16)
    return high, middle, (rest - middle.astype(f32)).astype(bf16)


def one_hot(mask):
    return jnp.where(mask, 1.0, 0.0).astype(bf16)


def exact_nn(hot, x):
    high, middle, low = split3(x)
    return nn(hot, high) + nn(hot, middle) + nn(hot, low)


def exact_nt(hot, x):
    high, middle, low = split3(x)
    return nt(hot, high) + nt(hot, middle) + nt(hot, low)


def column_of(row):
    return jnp.broadcast_to(row, (128, row.shape[1])).T[:, 0:1]


def iota(shape, dim):
    return lax.broadcasted_iota(i32, shape, dim)


def shift_of(value):
    assert value & (value - 1) == 0
    return value.bit_length() - 1


def right(value, bits):
    return lax.shift_right_logical(value, jnp.full(jnp.shape(value), bits, i32))


def order_of(rows, tile_rows, obs):
    tile = right(rows, shift_of(tile_rows))
    key = (tile * obs + iota((1, obs), 1)).astype(f32)
    rank = jnp.sum(jnp.where(column_of(key) < key, 1.0, 0.0), axis=0, keepdims=True)
    rank = rank.astype(i32)
    return tile, rank


def par_kernel(dims, where_ref, index_ref, values_ref, var_ref, noise_ref, par_ref, noise_out_ref):
    bin_rows, tile_rows, cols = dims
    batches, obs = index_ref.shape
    for b in range(batches):
        rows = index_ref[b:b + 1, :]
        _, rank = order_of(rows, tile_rows, obs)
        placed = (rank & (cols - 1)) * (obs // cols) + right(rank, shift_of(cols))
        hot = one_hot(iota((obs, obs), 0) == placed)
        par = jnp.concatenate(
            [right(rows, shift_of(bin_rows)).astype(f32), values_ref[b:b + 1, :],
             var_ref[b:b + 1, :], jnp.zeros((13, obs), f32), noise_ref[b]], axis=0)
        count = par.shape[0]
        moved = nt(jnp.concatenate(split3(par), axis=0), hot)
        moved = moved[0:count] + moved[count:2 * count] + moved[2 * count:]
        par_ref[4 * b:4 * b + 4, :] = moved[0:4]
        noise_out_ref[b] = moved[16:]


def send_kernel(dims, where_ref, index_ref, state_ref, send_ref):
    tile_rows, _, cols = dims
    _, rows_dev = state_ref.shape
    batches, obs = index_ref.shape
    my_tile, first = where_ref[0], where_ref[1]
    slots = send_ref.shape[0]
    per_col = slots // cols
    pick = jnp.zeros((slots, rows_dev), f32)
    for b in range(batches):
        rows = index_ref[b:b + 1, :]
        tile, rank = order_of(rows, tile_rows, obs)
        col = rank & (cols - 1)
        start = jnp.sum(jnp.where(tile < my_tile, 1.0, 0.0), axis=1, keepdims=True).astype(i32)
        base = start + ((col - start) & (cols - 1))
        place = right(rank - base + cols * obs, shift_of(cols)) - obs
        local = rows - first
        inside = (local >= 0) & (local < rows_dev) & (place >= 0) & (place < SLOTS)
        slot = jnp.where(inside, col * per_col + b * SLOTS + place, -1)
        pick += nt(one_hot(iota((slots, obs), 0) == slot),
                   one_hot(iota((rows_dev, obs), 0) == local))
    send_ref[...] = exact_nt(pick.astype(bf16), state_ref[...])


def dense_kernel(dims, where_ref, index_ref, state_ref, send_ref):
    tile_rows, _, cols, each_row = dims
    _, rows_dev = state_ref.shape
    batches, obs = index_ref.shape
    width = 128
    spots = []
    for b in range(batches):
        rows = index_ref[b:b + 1, :]
        _, rank = order_of(rows, tile_rows, obs)
        item = b * (obs // cols) + right(rank, shift_of(cols))
        spot = right(item, shift_of(each_row)) * (cols * each_row)
        spot = spot + (rank & (cols - 1)) * each_row + (item & (each_row - 1))
        spots.append((spot, one_hot(iota((rows_dev, obs), 0) == rows - where_ref[1])))

    def part(ds, at, carry):
        pick = jnp.zeros((width, rows_dev), f32)
        for spot, local in spots:
            pick += nt(one_hot(iota((width, obs), 0) + at == spot), local)
        send_ref[ds, :] = exact_nt(pick.astype(bf16), state_ref[...])
        return carry

    pieces(send_ref.shape[0], width, part)


def place_kernel(dims, where_ref, index_ref, slots_ref, out_ref):
    tile_rows, cols, sizes = dims
    batches, _ = index_ref.shape
    slots = slots_ref.shape[0]
    my_col = where_ref[0]
    mine = [where_ref[1 + k] for k in range(3)]
    half = out_ref.shape[0] // batches
    p = iota((slots, 1), 0)
    block = right(p, shift_of(batches * SLOTS))
    batch = right(p, shift_of(SLOTS)) & (batches - 1)
    slot = p & (SLOTS - 1)
    nx, nz, nc = sizes
    block_z = block & (nz - 1)
    block_x = right(block, shift_of(nz)) & (nx - 1)
    block_c = right(block, shift_of(nz * nx))
    tile_p = (((mine[0] - block_x) & (nx - 1)) * nz + ((mine[1] - block_z) & (nz - 1))) * nc
    tile_p = tile_p + ((mine[2] - block_c) & (nc - 1))
    start = jnp.zeros((slots, 1), i32)
    end = jnp.zeros((slots, 1), i32)
    for b in range(batches):
        tile = right(index_ref[b:b + 1, :], shift_of(tile_rows))
        before = jnp.sum(jnp.where(tile < tile_p, 1.0, 0.0), axis=1, keepdims=True).astype(i32)
        through = jnp.sum(jnp.where(tile <= tile_p, 1.0, 0.0), axis=1, keepdims=True).astype(i32)
        start = jnp.where(batch == b, before, start)
        end = jnp.where(batch == b, through, end)
    rank = start + ((my_col - start) & (cols - 1)) + slot * cols
    j = right(rank - my_col, shift_of(cols)) - mine[2] * half
    target = jnp.where((rank < end) & (j >= 0) & (j < half), batch * half + j, -1)
    wide = 128
    hot = jnp.where(iota((slots, wide), 1) == target, 1.0, 0.0).T.astype(bf16)
    out_ref[...] = exact_nn(hot[0:out_ref.shape[0]], slots_ref[...])


def taper(first, second):
    scaled = (first - second) * (1.0 / RADIUS)
    return jnp.exp(-0.5 * scaled * scaled)


def put_in_place(where, source_a, source_b, target, skip, stride, nzl, ny):
    zl, y, core = where
    unit = target.shape[0] // (2 * nzl * ny)

    def step(k, carry):
        dy, dz = right(k, shift_of(nzl)), k & (nzl - 1)
        at = ((zl - dz) & (nzl - 1)) * ny + ((y - dy) & (ny - 1))
        begin = pl.ds(pl.multiple_of((k * stride + skip) * unit, unit), unit)
        for source, half in ((source_a, core), (source_b, 1 - core)):
            to = pl.multiple_of((at * 2 + half) * unit, unit)
            target[pl.ds(to, unit), :] = source[begin, :]
        return carry

    lax.fori_loop(0, nzl * ny, step, 0)


def pieces(size, width, body, carry=0):
    def step(k, carry):
        at = k * width
        return body(pl.ds(pl.multiple_of(at, width), width), at, carry)

    return lax.fori_loop(0, size // width, step, carry)


def loop(size, width, body):
    def step(ds, at, carry):
        body(ds, at)
        return carry

    pieces(size, width, step)


def each(size, width, body):
    for at in range(0, size, width):
        body(slice(at, at + width), at)


def eye_part(obs, width, at):
    return iota((obs, width), 0) == iota((obs, width), 1) + at


def ident_part(obs, width, at):
    return jnp.where(eye_part(obs, width, at), 1.0, 0.0)


def centre(o, high, middle, low):
    def rows(ds, at):
        part = o[ds, :]
        part = part - jnp.mean(part, axis=1, keepdims=True)
        high[ds, :], middle[ds, :], low[ds, :] = split3(part)

    loop(o.shape[0], 128, rows)


def invert(pos_r, var_r, pos_c, members, high, middle, low, left, gram, other, spare, s_high, s_low,
           xa, xb, ra, rb, eh, el, vec):
    obs = gram.shape[0]
    width = obs
    norming = 1.0 / (members - 1)

    def cross_terms(ds, at):
        left[:, ds] = nt(high[...], middle[ds, :]) + nt(high[...], low[ds, :])

    each(obs, width, cross_terms)

    def covariance(ds, at):
        product = nt(high[...], high[ds, :]) + nt(middle[...], middle[ds, :])
        product = product + left[:, ds] + left[ds, :].T
        eye = eye_part(obs, width, at)
        covar = taper(pos_c, pos_r[:, ds]) * product * norming + jnp.where(eye, var_r[:, ds], 0.0)
        gram[:, ds] = covar
        vec[0:1, ds] = lax.rsqrt(jnp.sum(jnp.where(eye, covar, 0.0), axis=0, keepdims=True))

    each(obs, width, covariance)
    scale_c = column_of(vec[0:1, :])

    def rescale(ds, at):
        scaled = gram[:, ds] * scale_c * vec[0:1, ds]
        gram[:, ds] = scaled
        s_high[:, ds], s_low[:, ds] = split2(scaled)

    loop(obs, 128, rescale)

    def squared(ds, at):
        square = nn(s_high[...], s_high[:, ds])
        left[:, ds] = square
        vec[1:2, ds] = jnp.sum(jnp.abs(square), axis=0, keepdims=True)

    each(obs, width, squared)
    upper = jnp.sqrt(jnp.max(vec[1:2, :], axis=1, keepdims=True)) * 1.01
    lower = jnp.min(var_r[...] * vec[0:1, :] * vec[0:1, :], axis=1, keepdims=True)
    alpha = 2.0 / (upper + lower)

    def widen(low_end):
        image = low_end * (2.0 - low_end)
        factor = 2.0 / (1.0 + image)
        return factor, factor * image

    factor, low_end = widen(alpha * lower)

    def first(ds, at):
        ident = ident_part(obs, 128, at)
        step = alpha * gram[:, ds]
        xa[:, ds] = (factor * alpha * (2.0 * ident - step)).astype(bf16)
        ra[:, ds] = (ident - factor * (2.0 * step - alpha * alpha * left[:, ds])).astype(bf16)

    loop(obs, 128, first)

    def grow(old, new, factor):
        def part(ds, at):
            new[:, ds] = (factor * (old[:, ds].astype(f32) + nn(old[...], ra[:, ds]))).astype(bf16)

        each(obs, width, part)

    def remain(new):
        def part(ds, at):
            ra[:, ds] = (ident_part(obs, width, at) - nn(s_high[...], new[:, ds])).astype(bf16)

        each(obs, width, part)

    factor, low_end = widen(low_end)
    grow(xa, xb, factor)
    remain(xb)
    factor, low_end = widen(low_end)
    grow(xb, xa, factor)
    remain(xa)
    factor, low_end = widen(low_end)
    grow(xa, xb, factor)

    def remain_last(ds, at):
        residual = (ident_part(obs, width, at)
                    - nn(s_high[...], xb[:, ds]) - nn(s_low[...], xb[:, ds]))
        left[:, ds] = residual
        ra[:, ds] = residual.astype(bf16)
        vec[1:2, ds] = jnp.sum(jnp.abs(residual), axis=0, keepdims=True)

    each(obs, width, remain_last)

    def second_order(ds, at):
        rb[:, ds] = (left[:, ds] + nn(ra[...], ra[:, ds])).astype(bf16)

    each(obs, width, second_order)

    def correction(ds, at):
        eh[:, ds], el[:, ds] = split2(nn(xb[...], rb[:, ds]))

    each(obs, width, correction)
    size = jnp.max(vec[1:2, :], axis=1, keepdims=True)

    @pl.when(jnp.logical_not(size[0, 0] < 0.1))
    def _():
        narrow = 128
        full = functools.partial(jnp.dot, precision=lax.Precision.HIGHEST,
                                 preferred_element_type=f32)
        sums = jnp.sum(jnp.abs(gram[...]), axis=0, keepdims=True)
        guess = 1.0 / jnp.max(sums, axis=1, keepdims=True)

        def start(ds, at):
            left[:, ds] = ident_part(obs, narrow, at) * guess

        loop(obs, narrow, start)

        def blocks(body, carry):
            def across(ds, at, carry):
                return pieces(obs, narrow, lambda dr, ar, c: body(dr, ar, ds, at, c), carry)

            return pieces(obs, narrow, across, carry)

        def advance(carry):
            def residuals(dr, ar, ds, at, error):
                eye = iota((narrow, narrow), 0) + ar == iota((narrow, narrow), 1) + at
                residual = jnp.where(eye, 1.0, 0.0) - full(gram[dr, :], left[:, ds])
                other[dr, ds] = residual
                return error + jnp.sum(residual * residual)

            def update(dr, ar, ds, at, carry):
                spare[dr, ds] = left[dr, ds] + full(left[dr, :], other[:, ds])
                return carry

            error = blocks(residuals, jnp.float32(0.0))
            blocks(update, 0)
            left[...] = spare[...]
            return carry[0] + 1, error

        lax.while_loop(lambda c: (c[0] < 40) & jnp.logical_not(c[1] < 1e-7), advance,
                       (jnp.int32(0), jnp.float32(1.0)))
        xb[...] = left[...].astype(bf16)
        eh[...], el[...] = split2(left[...] - xb[...].astype(f32))


def innovate(val_r, var_r, scale_r, o, n, vh, vl):
    deviation = jnp.sqrt(var_r)

    def rows(ds, at):
        part = val_r + deviation * n[ds, :] - o[:, ds].T
        vh[ds, :], vl[ds, :] = split2(part * scale_r)

    loop(n.shape[0], 128, rows)


def weigh(pos_c, pos_dev, x, high, middle, members):
    xh, xl = split2(x - jnp.mean(x, axis=0, keepdims=True))
    cross = nn(high[...], xh) + nn(high[...], xl) + nn(middle[...], xh)
    return taper(pos_c, pos_dev) * cross * (1.0 / (members - 1))


def columns(par_ref):
    return jnp.concatenate([par_ref[...], jnp.zeros((120, par_ref.shape[1]), f32)], axis=0).T


def own_positions(first, rows_dev, bin_rows):
    return right(first + iota((1, rows_dev), 1), shift_of(bin_rows)).astype(f32)


def main_kernel(dims, where_ref, par_ref, oa, ob, na, nb, x_ref, out_ref,
                high0, middle0, high, middle, o0, o, n, vh, vl, sh, sl, xb, eh, el, vec, *work):
    bin_rows, nzl, ny = dims
    where = [where_ref[k] for k in range(3)]
    obs, members = o.shape
    low, left, gram, other, spare, s_high, s_low, xa, ra, rb = work
    cols_par = columns(par_ref)
    pos_dev = own_positions(where_ref[3], x_ref.shape[1], bin_rows)
    norming = 1.0 / (members - 1)
    put_in_place(where, oa, ob, o0, 0, 2, nzl, ny)
    put_in_place(where, na, nb, n, 0, 2, nzl, ny)
    pos_c = cols_par[:, 0:1]
    centre(o0, high0, middle0, low)
    invert(par_ref.at[0:1], par_ref.at[2:3], pos_c, members, high0, middle0, low, left, gram,
           other, spare, s_high, s_low, xa, xb, ra, rb, eh, el, vec)
    innovate(par_ref[1:2, :], par_ref[2:3, :], vec[0:1, :], o0, n, vh, vl)
    solved = nn(vh[...], xb[...]) + nn(vl[...], xb[...]) + nn(vh[...], eh[...])
    solved = solved + nn(vh[...], el[...])
    sh[...], sl[...] = split2(solved * vec[0:1, :])
    wh, wl = split2(weigh(pos_c, pos_dev, x_ref[...], high0, middle0, members))
    out_ref[...] = x_ref[...] + nn(sh[...], wh) + nn(sh[...], wl) + nn(sl[...], wh)
    put_in_place(where, oa, ob, o, 1, 2, nzl, ny)
    put_in_place(where, na, nb, n, 1, 2, nzl, ny)
    pos_c = cols_par[:, 4:5]
    centre(o, high, middle, low)

    def weights(ds, at):
        cross = nt(high[...], high0[ds, :]) + nt(high[...], middle0[ds, :])
        cross = cross + nt(middle[...], high0[ds, :])
        xa[:, ds], xb[:, ds] = split2(taper(pos_c, par_ref[0:1, ds]) * cross * norming)

    each(obs, obs, weights)

    def update(ds, at):
        o[:, ds] = (o[:, ds] + nt(xa[...], sh[ds, :]) + nt(xa[...], sl[ds, :])
                    + nt(xb[...], sh[ds, :]))

    each(members, members, update)
    centre(o, high, middle, low)
    invert(par_ref.at[4:5], par_ref.at[6:7], pos_c, members, high, middle, low, left, gram, other,
           spare, s_high, s_low, xa, xb, ra, rb, eh, el, vec)
    scale_c = column_of(vec[0:1, :])
    wh, wl = split2(weigh(pos_c, pos_dev, out_ref[...], high, middle, members) * scale_c)
    applied = nn(xb[...], wh) + nn(xb[...], wl) + nn(eh[...], wh) + nn(el[...], wh)
    wh, wl = split2(applied * scale_c)
    innovate(par_ref[5:6, :], par_ref[6:7, :], jnp.ones((1, obs), f32), o, n, vh, vl)
    out_ref[...] = out_ref[...] + nn(vh[...], wh) + nn(vh[...], wl) + nn(vl[...], wh)


def ring_gather(value, axis, size):
    parts = [value] + [
        lax.ppermute(value, axis, [(i, (i + k) % size) for i in range(size)])
        for k in range(1, size)
    ]
    return jnp.concatenate(parts, axis=0)


def on_device(state, obs_index, obs_values, obs_var, noise):
    members, rows_dev = state.shape
    batches, obs = obs_index.shape
    cols = lax.axis_size(COL)
    nx, nz, nc = (lax.axis_size(a) for a in ROW)
    nzl, ny = (lax.axis_size(a) for a in COL)
    my_col = lax.axis_index(COL)
    my_tile = lax.axis_index(ROW)
    tile_rows = rows_dev * cols
    bin_rows = tile_rows * nx * nz * nc // POSITIONS
    first = (my_tile * cols + my_col) * rows_dev
    core = lax.axis_index("core")
    noise = jnp.swapaxes(noise, 1, 2)
    slots = cols * batches * SLOTS
    unit = obs // cols // nc
    prep_dims = (tile_rows, bin_rows, cols)

    def scalars(*values):
        return jnp.stack([jnp.asarray(v, i32) for v in values])

    smem = pl.BlockSpec(memory_space=pltpu.SMEM)
    vmem = pl.BlockSpec(memory_space=pltpu.VMEM)

    def call(kernel, shapes, inputs, scratch=(), flops=0, room=16):
        return pl.pallas_call(
            kernel,
            out_shape=shapes,
            in_specs=[smem] + [vmem] * (len(inputs) - 1),
            out_specs=jax.tree.map(lambda _: vmem, shapes),
            scratch_shapes=list(scratch),
            cost_estimate=pl.CostEstimate(flops=flops, bytes_accessed=4 << 20, transcendentals=0),
            compiler_params=pltpu.CompilerParams(vmem_limit_bytes=room << 20),
        )(*inputs)

    send = call(
        functools.partial(send_kernel, prep_dims),
        jax.ShapeDtypeStruct((slots, members), f32),
        (scalars(my_tile, first), obs_index, state), flops=1 << 28)
    mine = lax.all_to_all(send.reshape(cols, batches * SLOTS, members), COL, 0, 0, tiled=True)
    par, noise_t = call(
        functools.partial(par_kernel, (bin_rows, tile_rows, cols)),
        (jax.ShapeDtypeStruct((4 * batches, obs), f32),
         jax.ShapeDtypeStruct(noise.shape, f32)),
        (scalars(0), obs_index, obs_values, obs_var, noise), flops=1 << 30)
    mine = jnp.sum(mine, axis=0)
    mine = ring_gather(mine, "zh", nz)
    mine = ring_gather(mine, "x", nx)
    mine = ring_gather(mine, "core", nc)
    held = call(
        functools.partial(place_kernel, (tile_rows, cols, (nx, nz, nc))),
        jax.ShapeDtypeStruct((batches * unit, members), f32),
        (scalars(my_col, *(lax.axis_index(a) for a in ROW)), obs_index, mine),
        flops=1 << 28)

    def dense(held):
        tiles_all = nx * nz * nc
        each_row = batches * obs // cols // tiles_all
        send = call(
            functools.partial(dense_kernel, prep_dims + (each_row,)),
            jax.ShapeDtypeStruct((batches * obs, members), f32),
            (scalars(my_tile, first), obs_index, state))
        mine = lax.all_to_all(
            send.reshape(tiles_all * cols, each_row, members), ROW_COL, 0, 0, tiled=True)
        mine = jnp.sum(mine, axis=0)
        copies = jnp.broadcast_to(mine, (tiles_all, *mine.shape))
        mine = lax.all_to_all(copies, ROW, 0, 0, tiled=True)
        mine = mine.reshape(batches, nc, unit, members)
        return lax.dynamic_index_in_dim(mine, core, 1, keepdims=False).reshape(held.shape)

    tiles = obs_index[:, :, None] // tile_rows == jnp.arange(nx * nz * nc, dtype=i32)
    crowded = jnp.max(jnp.sum(tiles.astype(i32), axis=1)) > cols * SLOTS
    held = lax.cond(crowded, dense, lambda held: held, held)

    swap = [(0, 1), (1, 0)]
    part = noise.shape[1] // nc
    noise_half = lax.dynamic_slice_in_dim(noise_t, core * part, part, axis=1)
    na = ring_gather(noise_half.reshape(batches * part, obs), "zl", nzl)
    na = ring_gather(na, "y", ny)
    nb = lax.ppermute(na, "core", swap)
    oa = ring_gather(held, "zl", nzl)
    oa = ring_gather(oa, "y", ny)
    ob = lax.ppermute(oa, "core", swap)
    full = (obs, members)
    wide, slim = pltpu.VMEM(full, f32), pltpu.VMEM(full, bf16)
    where = scalars(lax.axis_index("zl"), lax.axis_index("y"), core, first)
    return call(
        functools.partial(main_kernel, (bin_rows, nzl, ny)),
        jax.ShapeDtypeStruct(state.shape, f32),
        (where, par, oa, ob, na, nb, state),
        scratch=([slim] * 4 + [wide] * 3 + [slim] * 7 + [pltpu.VMEM((8, obs), f32)]
                 + [slim] + [wide] * 4 + [slim] * 5),
        flops=20 << 30, room=32)


def solution(mesh):
    split = Mesh(mesh.devices.reshape(4, 2, 2, 4, 4), ROW_COL)
    placed = (P(None, ROW_COL), P(), P(), P(), P(None, None, COL))

    return jax.shard_map(
        on_device, mesh=split, in_specs=placed, out_specs=P(None, ROW_COL), check_vma=False
    )
```

```python
import functools

import jax
import jax.numpy as jnp
from jax import lax
from jax.experimental import pallas as pl
from jax.experimental.pallas import tpu as pltpu
from jax.sharding import Mesh
from jax.sharding import PartitionSpec as P


POSITIONS = 256
RADIUS = 64
ROW = ("x", "zh", "core")
COL = ("zl", "y")
ROW_COL = ROW + COL
SLOTS = 4

f32 = jnp.float32
bf16 = jnp.bfloat16
i32 = jnp.int32


def nn(a, b):
    return lax.dot_general(a, b, (((1,), (0,)), ((), ())), preferred_element_type=f32)


def nt(a, b):
    return lax.dot_general(a, b, (((1,), (1,)), ((), ())), preferred_element_type=f32)


def split2(x):
    high = x.astype(bf16)
    return high, (x - high.astype(f32)).astype(bf16)


def split3(x):
    high = x.astype(bf16)
    rest = x - high.astype(f32)
    middle = rest.astype(bf16)
    return high, middle, (rest - middle.astype(f32)).astype(bf16)


def one_hot(mask):
    return jnp.where(mask, 1.0, 0.0).astype(bf16)


def exact_nn(hot, x):
    high, middle, low = split3(x)
    return nn(hot, high) + nn(hot, middle) + nn(hot, low)


def exact_nt(hot, x):
    high, middle, low = split3(x)
    return nt(hot, high) + nt(hot, middle) + nt(hot, low)


def column_of(row):
    return jnp.broadcast_to(row, (128, row.shape[1])).T[:, 0:1]


def iota(shape, dim):
    return lax.broadcasted_iota(i32, shape, dim)


def shift_of(value):
    assert value & (value - 1) == 0
    return value.bit_length() - 1


def right(value, bits):
    return lax.shift_right_logical(value, jnp.full(jnp.shape(value), bits, i32))


def order_of(rows, tile_rows, obs):
    tile = right(rows, shift_of(tile_rows))
    key = (tile * obs + iota((1, obs), 1)).astype(f32)
    rank = jnp.sum(jnp.where(column_of(key) < key, 1.0, 0.0), axis=0, keepdims=True)
    rank = rank.astype(i32)
    return tile, rank


def par_kernel(dims, where_ref, index_ref, values_ref, var_ref, noise_ref, par_ref, noise_out_ref):
    bin_rows, tile_rows, cols = dims
    batches, obs = index_ref.shape
    for b in range(batches):
        rows = index_ref[b:b + 1, :]
        _, rank = order_of(rows, tile_rows, obs)
        placed = (rank & (cols - 1)) * (obs // cols) + right(rank, shift_of(cols))
        hot = one_hot(iota((obs, obs), 0) == placed)
        par = jnp.concatenate(
            [right(rows, shift_of(bin_rows)).astype(f32), values_ref[b:b + 1, :],
             var_ref[b:b + 1, :], jnp.zeros((13, obs), f32), noise_ref[b]], axis=0)
        count = par.shape[0]
        moved = nt(jnp.concatenate(split3(par), axis=0), hot)
        moved = moved[0:count] + moved[count:2 * count] + moved[2 * count:]
        par_ref[4 * b:4 * b + 4, :] = moved[0:4]
        noise_out_ref[b] = moved[16:]


def send_kernel(dims, where_ref, index_ref, state_ref, send_ref):
    tile_rows, _, cols = dims
    _, rows_dev = state_ref.shape
    batches, obs = index_ref.shape
    my_tile, first = where_ref[0], where_ref[1]
    slots = send_ref.shape[0]
    per_col = slots // cols
    pick = jnp.zeros((slots, rows_dev), f32)
    for b in range(batches):
        rows = index_ref[b:b + 1, :]
        tile, rank = order_of(rows, tile_rows, obs)
        col = rank & (cols - 1)
        start = jnp.sum(jnp.where(tile < my_tile, 1.0, 0.0), axis=1, keepdims=True).astype(i32)
        base = start + ((col - start) & (cols - 1))
        place = right(rank - base + cols * obs, shift_of(cols)) - obs
        local = rows - first
        inside = (local >= 0) & (local < rows_dev) & (place >= 0) & (place < SLOTS)
        slot = jnp.where(inside, col * per_col + b * SLOTS + place, -1)
        pick += nt(one_hot(iota((slots, obs), 0) == slot),
                   one_hot(iota((rows_dev, obs), 0) == local))
    send_ref[...] = exact_nt(pick.astype(bf16), state_ref[...])


def dense_kernel(dims, where_ref, index_ref, state_ref, send_ref):
    tile_rows, _, cols, each_row = dims
    _, rows_dev = state_ref.shape
    batches, obs = index_ref.shape
    width = 128
    spots = []
    for b in range(batches):
        rows = index_ref[b:b + 1, :]
        _, rank = order_of(rows, tile_rows, obs)
        item = b * (obs // cols) + right(rank, shift_of(cols))
        spot = right(item, shift_of(each_row)) * (cols * each_row)
        spot = spot + (rank & (cols - 1)) * each_row + (item & (each_row - 1))
        spots.append((spot, one_hot(iota((rows_dev, obs), 0) == rows - where_ref[1])))

    def part(ds, at, carry):
        pick = jnp.zeros((width, rows_dev), f32)
        for spot, local in spots:
            pick += nt(one_hot(iota((width, obs), 0) + at == spot), local)
        send_ref[ds, :] = exact_nt(pick.astype(bf16), state_ref[...])
        return carry

    pieces(send_ref.shape[0], width, part)


def place_kernel(dims, where_ref, index_ref, slots_ref, out_ref):
    tile_rows, cols, sizes = dims
    batches, _ = index_ref.shape
    slots = slots_ref.shape[0]
    my_col = where_ref[0]
    mine = [where_ref[1 + k] for k in range(3)]
    half = out_ref.shape[0] // batches
    p = iota((slots, 1), 0)
    block = right(p, shift_of(batches * SLOTS))
    batch = right(p, shift_of(SLOTS)) & (batches - 1)
    slot = p & (SLOTS - 1)
    nx, nz, nc = sizes
    block_z = block & (nz - 1)
    block_x = right(block, shift_of(nz)) & (nx - 1)
    block_c = right(block, shift_of(nz * nx))
    tile_p = (((mine[0] - block_x) & (nx - 1)) * nz + ((mine[1] - block_z) & (nz - 1))) * nc
    tile_p = tile_p + ((mine[2] - block_c) & (nc - 1))
    start = jnp.zeros((slots, 1), i32)
    end = jnp.zeros((slots, 1), i32)
    for b in range(batches):
        tile = right(index_ref[b:b + 1, :], shift_of(tile_rows))
        before = jnp.sum(jnp.where(tile < tile_p, 1.0, 0.0), axis=1, keepdims=True).astype(i32)
        through = jnp.sum(jnp.where(tile <= tile_p, 1.0, 0.0), axis=1, keepdims=True).astype(i32)
        start = jnp.where(batch == b, before, start)
        end = jnp.where(batch == b, through, end)
    rank = start + ((my_col - start) & (cols - 1)) + slot * cols
    j = right(rank - my_col, shift_of(cols)) - mine[2] * half
    target = jnp.where((rank < end) & (j >= 0) & (j < half), batch * half + j, -1)
    wide = 128
    hot = jnp.where(iota((slots, wide), 1) == target, 1.0, 0.0).T.astype(bf16)
    out_ref[...] = exact_nn(hot[0:out_ref.shape[0]], slots_ref[...])


def taper(first, second):
    scaled = (first - second) * (1.0 / RADIUS)
    return jnp.exp(-0.5 * scaled * scaled)


def put_in_place(where, source_a, source_b, target, skip, stride, nzl, ny):
    zl, y, core = where
    unit = target.shape[0] // (2 * nzl * ny)

    for k in range(nzl * ny):
        dy, dz = divmod(k, nzl)
        at = ((zl - dz) & (nzl - 1)) * ny + ((y - dy) & (ny - 1))
        begin = (k * stride + skip) * unit
        for source, half in ((source_a, core), (source_b, 1 - core)):
            to = pl.multiple_of((at * 2 + half) * unit, unit)
            target[pl.ds(to, unit), :] = source[begin:begin + unit, :]


def pieces(size, width, body, carry=0):
    def step(k, carry):
        at = k * width
        return body(pl.ds(pl.multiple_of(at, width), width), at, carry)

    return lax.fori_loop(0, size // width, step, carry)


def loop(size, width, body):
    def step(ds, at, carry):
        body(ds, at)
        return carry

    pieces(size, width, step)


def each(size, width, body):
    for at in range(0, size, width):
        body(slice(at, at + width), at)


def eye_part(obs, width, at):
    return iota((obs, width), 0) == iota((obs, width), 1) + at


def ident_part(obs, width, at):
    return jnp.where(eye_part(obs, width, at), 1.0, 0.0)


def centre(o, high, middle):
    def rows(ds, at):
        part = o[ds, :]
        part = part - jnp.mean(part, axis=1, keepdims=True)
        high[ds, :], middle[ds, :] = split2(part)

    each(o.shape[0], 128, rows)


def invert(pos_r, var_r, pos_c, members, high, middle, left, gram, other, spare, s_high, s_low,
           xa, xb, ra, rb, eh, vec):
    obs = gram.shape[0]
    width = obs
    norming = 1.0 / (members - 1)

    def cross_terms(ds, at):
        left[:, ds] = nt(high[...], middle[ds, :])

    each(obs, width, cross_terms)

    def covariance(ds, at):
        product = nt(high[...], high[ds, :]) + left[:, ds] + left[ds, :].T
        eye = eye_part(obs, width, at)
        covar = taper(pos_c, pos_r[:, ds]) * product * norming + jnp.where(eye, var_r[:, ds], 0.0)
        gram[:, ds] = covar
        vec[0:1, ds] = lax.rsqrt(jnp.sum(jnp.where(eye, covar, 0.0), axis=0, keepdims=True))

    each(obs, width, covariance)
    scale_c = column_of(vec[0:1, :])

    def rescale(ds, at):
        scaled = gram[:, ds] * scale_c * vec[0:1, ds]
        gram[:, ds] = scaled
        s_high[:, ds], s_low[:, ds] = split2(scaled)

    each(obs, 128, rescale)

    def squared(ds, at):
        square = nn(s_high[...], s_high[:, ds])
        left[:, ds] = square
        vec[1:2, ds] = jnp.sum(jnp.abs(square), axis=0, keepdims=True)

    each(obs, width, squared)
    upper = jnp.sqrt(jnp.max(vec[1:2, :], axis=1, keepdims=True)) * 1.01
    lower = jnp.min(var_r[...] * vec[0:1, :] * vec[0:1, :], axis=1, keepdims=True)
    alpha = 2.0 / (upper + lower)

    def widen(low_end):
        image = low_end * (2.0 - low_end)
        factor = 2.0 / (1.0 + image)
        return factor, factor * image

    factor, low_end = widen(alpha * lower)

    def first(ds, at):
        ident = ident_part(obs, 128, at)
        step = alpha * gram[:, ds]
        xa[:, ds] = (factor * alpha * (2.0 * ident - step)).astype(bf16)
        ra[:, ds] = (ident - factor * (2.0 * step - alpha * alpha * left[:, ds])).astype(bf16)

    each(obs, 128, first)

    def grow(old, new, factor):
        def part(ds, at):
            new[:, ds] = (factor * (old[:, ds].astype(f32) + nn(old[...], ra[:, ds]))).astype(bf16)

        each(obs, width, part)

    def remain(new):
        def part(ds, at):
            ra[:, ds] = (ident_part(obs, width, at) - nn(s_high[...], new[:, ds])).astype(bf16)

        each(obs, width, part)

    factor, low_end = widen(low_end)
    grow(xa, xb, factor)
    remain(xb)
    factor, low_end = widen(low_end)
    grow(xb, xa, factor)
    remain(xa)
    factor, low_end = widen(low_end)
    grow(xa, xb, factor)

    def remain_last(ds, at):
        residual = (ident_part(obs, width, at)
                    - nn(s_high[...], xb[:, ds]) - nn(s_low[...], xb[:, ds]))
        left[:, ds] = residual
        ra[:, ds] = residual.astype(bf16)
        vec[1:2, ds] = jnp.sum(jnp.abs(residual), axis=0, keepdims=True)

    each(obs, width, remain_last)

    def second_order(ds, at):
        rb[:, ds] = (left[:, ds] + nn(ra[...], ra[:, ds])).astype(bf16)

    each(obs, width, second_order)

    def correction(ds, at):
        eh[:, ds] = nn(xb[...], rb[:, ds]).astype(bf16)

    each(obs, width, correction)
    size = jnp.max(vec[1:2, :], axis=1, keepdims=True)

    @pl.when(jnp.logical_not(size[0, 0] < 0.1))
    def _():
        narrow = 128
        full = functools.partial(jnp.dot, precision=lax.Precision.HIGHEST,
                                 preferred_element_type=f32)
        sums = jnp.sum(jnp.abs(gram[...]), axis=0, keepdims=True)
        guess = 1.0 / jnp.max(sums, axis=1, keepdims=True)

        def start(ds, at):
            left[:, ds] = ident_part(obs, narrow, at) * guess

        loop(obs, narrow, start)

        def blocks(body, carry):
            def across(ds, at, carry):
                return pieces(obs, narrow, lambda dr, ar, c: body(dr, ar, ds, at, c), carry)

            return pieces(obs, narrow, across, carry)

        def advance(carry):
            def residuals(dr, ar, ds, at, error):
                eye = iota((narrow, narrow), 0) + ar == iota((narrow, narrow), 1) + at
                residual = jnp.where(eye, 1.0, 0.0) - full(gram[dr, :], left[:, ds])
                other[dr, ds] = residual
                return error + jnp.sum(residual * residual)

            def update(dr, ar, ds, at, carry):
                spare[dr, ds] = left[dr, ds] + full(left[dr, :], other[:, ds])
                return carry

            error = blocks(residuals, jnp.float32(0.0))
            blocks(update, 0)
            left[...] = spare[...]
            return carry[0] + 1, error

        lax.while_loop(lambda c: (c[0] < 40) & jnp.logical_not(c[1] < 1e-7), advance,
                       (jnp.int32(0), jnp.float32(1.0)))
        xb[...] = left[...].astype(bf16)
        eh[...] = (left[...] - xb[...].astype(f32)).astype(bf16)


def innovate(val_r, var_r, scale_r, o, n, vh, vl):
    deviation = jnp.sqrt(var_r)

    def rows(ds, at):
        part = val_r + deviation * n[ds, :] - o[:, ds].T
        vh[ds, :], vl[ds, :] = split2(part * scale_r)

    each(n.shape[0], 128, rows)


def weigh(pos_c, pos_dev, x, high, middle, members):
    xh, xl = split2(x - jnp.mean(x, axis=0, keepdims=True))
    cross = nn(high[...], xh) + nn(high[...], xl) + nn(middle[...], xh)
    return taper(pos_c, pos_dev) * cross * (1.0 / (members - 1))


def columns(par_ref):
    return jnp.concatenate([par_ref[...], jnp.zeros((120, par_ref.shape[1]), f32)], axis=0).T


def own_positions(first, rows_dev, bin_rows):
    return right(first + iota((1, rows_dev), 1), shift_of(bin_rows)).astype(f32)


def main_kernel(dims, where_ref, par_ref, oa, ob, na, nb, x_ref, out_ref,
                high0, middle0, high, middle, o0, o, n, vh, vl, sh, sl, xb, eh, vec, *work):
    bin_rows, nzl, ny = dims
    where = [where_ref[k] for k in range(3)]
    obs, members = o.shape
    left, gram, other, spare, s_high, s_low, xa, ra, rb = work
    cols_par = columns(par_ref)
    pos_dev = own_positions(where_ref[3], x_ref.shape[1], bin_rows)
    norming = 1.0 / (members - 1)
    put_in_place(where, oa, ob, o0, 0, 2, nzl, ny)
    put_in_place(where, na, nb, n, 0, 2, nzl, ny)
    pos_c = cols_par[:, 0:1]
    centre(o0, high0, middle0)
    invert(par_ref.at[0:1], par_ref.at[2:3], pos_c, members, high0, middle0, left, gram,
           other, spare, s_high, s_low, xa, xb, ra, rb, eh, vec)
    innovate(par_ref[1:2, :], par_ref[2:3, :], vec[0:1, :], o0, n, vh, vl)
    solved = nn(vh[...], xb[...]) + nn(vl[...], xb[...]) + nn(vh[...], eh[...])
    sh[...], sl[...] = split2(solved * vec[0:1, :])
    wh, wl = split2(weigh(pos_c, pos_dev, x_ref[...], high0, middle0, members))
    out_ref[...] = x_ref[...] + nn(sh[...], wh) + nn(sh[...], wl) + nn(sl[...], wh)
    put_in_place(where, oa, ob, o, 1, 2, nzl, ny)
    put_in_place(where, na, nb, n, 1, 2, nzl, ny)
    pos_c = cols_par[:, 4:5]
    centre(o, high, middle)

    def weights(ds, at):
        cross = nt(high[...], high0[ds, :]) + nt(high[...], middle0[ds, :])
        cross = cross + nt(middle[...], high0[ds, :])
        xa[:, ds], xb[:, ds] = split2(taper(pos_c, par_ref[0:1, ds]) * cross * norming)

    each(obs, obs, weights)

    def update(ds, at):
        o[:, ds] = (o[:, ds] + nt(xa[...], sh[ds, :]) + nt(xa[...], sl[ds, :])
                    + nt(xb[...], sh[ds, :]))

    each(members, members, update)
    centre(o, high, middle)
    invert(par_ref.at[4:5], par_ref.at[6:7], pos_c, members, high, middle, left, gram, other,
           spare, s_high, s_low, xa, xb, ra, rb, eh, vec)
    scale_c = column_of(vec[0:1, :])
    wh, wl = split2(weigh(pos_c, pos_dev, out_ref[...], high, middle, members) * scale_c)
    applied = nn(xb[...], wh) + nn(xb[...], wl) + nn(eh[...], wh)
    wh, wl = split2(applied * scale_c)
    innovate(par_ref[5:6, :], par_ref[6:7, :], jnp.ones((1, obs), f32), o, n, vh, vl)
    out_ref[...] = out_ref[...] + nn(vh[...], wh) + nn(vh[...], wl) + nn(vl[...], wh)


def ring_gather(value, axis, size):
    parts = [value] + [
        lax.ppermute(value, axis, [(i, (i + k) % size) for i in range(size)])
        for k in range(1, size)
    ]
    return jnp.concatenate(parts, axis=0)


def on_device(state, obs_index, obs_values, obs_var, noise):
    members, rows_dev = state.shape
    batches, obs = obs_index.shape
    cols = lax.axis_size(COL)
    nx, nz, nc = (lax.axis_size(a) for a in ROW)
    nzl, ny = (lax.axis_size(a) for a in COL)
    my_col = lax.axis_index(COL)
    my_tile = lax.axis_index(ROW)
    tile_rows = rows_dev * cols
    bin_rows = tile_rows * nx * nz * nc // POSITIONS
    first = (my_tile * cols + my_col) * rows_dev
    core = lax.axis_index("core")
    noise = jnp.swapaxes(noise, 1, 2)
    slots = cols * batches * SLOTS
    unit = obs // cols // nc
    prep_dims = (tile_rows, bin_rows, cols)

    def scalars(*values):
        return jnp.stack([jnp.asarray(v, i32) for v in values])

    smem = pl.BlockSpec(memory_space=pltpu.SMEM)
    vmem = pl.BlockSpec(memory_space=pltpu.VMEM)

    def call(kernel, shapes, inputs, scratch=(), flops=0, room=16):
        return pl.pallas_call(
            kernel,
            out_shape=shapes,
            in_specs=[smem] + [vmem] * (len(inputs) - 1),
            out_specs=jax.tree.map(lambda _: vmem, shapes),
            scratch_shapes=list(scratch),
            cost_estimate=pl.CostEstimate(flops=flops, bytes_accessed=4 << 20, transcendentals=0),
            compiler_params=pltpu.CompilerParams(vmem_limit_bytes=room << 20),
        )(*inputs)

    send = call(
        functools.partial(send_kernel, prep_dims),
        jax.ShapeDtypeStruct((slots, members), f32),
        (scalars(my_tile, first), obs_index, state), flops=1 << 28)
    mine = lax.all_to_all(send.reshape(cols, batches * SLOTS, members), COL, 0, 0, tiled=True)
    par, noise_t = call(
        functools.partial(par_kernel, (bin_rows, tile_rows, cols)),
        (jax.ShapeDtypeStruct((4 * batches, obs), f32),
         jax.ShapeDtypeStruct(noise.shape, f32)),
        (scalars(0), obs_index, obs_values, obs_var, noise), flops=1 << 30)
    mine = jnp.sum(mine, axis=0)
    mine = ring_gather(mine, "zh", nz)
    mine = ring_gather(mine, "x", nx)
    mine = ring_gather(mine, "core", nc)
    held = call(
        functools.partial(place_kernel, (tile_rows, cols, (nx, nz, nc))),
        jax.ShapeDtypeStruct((batches * unit, members), f32),
        (scalars(my_col, *(lax.axis_index(a) for a in ROW)), obs_index, mine),
        flops=1 << 28)

    def dense(held):
        tiles_all = nx * nz * nc
        each_row = batches * obs // cols // tiles_all
        send = call(
            functools.partial(dense_kernel, prep_dims + (each_row,)),
            jax.ShapeDtypeStruct((batches * obs, members), f32),
            (scalars(my_tile, first), obs_index, state))
        mine = lax.all_to_all(
            send.reshape(tiles_all * cols, each_row, members), ROW_COL, 0, 0, tiled=True)
        mine = jnp.sum(mine, axis=0)
        copies = jnp.broadcast_to(mine, (tiles_all, *mine.shape))
        mine = lax.all_to_all(copies, ROW, 0, 0, tiled=True)
        mine = mine.reshape(batches, nc, unit, members)
        return lax.dynamic_index_in_dim(mine, core, 1, keepdims=False).reshape(held.shape)

    tiles = obs_index[:, :, None] // tile_rows == jnp.arange(nx * nz * nc, dtype=i32)
    crowded = jnp.max(jnp.sum(tiles.astype(i32), axis=1)) > cols * SLOTS
    held = lax.cond(crowded, dense, lambda held: held, held)

    swap = [(0, 1), (1, 0)]
    part = noise.shape[1] // nc
    noise_half = lax.dynamic_slice_in_dim(noise_t, core * part, part, axis=1)
    na = ring_gather(noise_half.reshape(batches * part, obs), "zl", nzl)
    na = ring_gather(na, "y", ny)
    nb = lax.ppermute(na, "core", swap)
    oa = ring_gather(held, "zl", nzl)
    oa = ring_gather(oa, "y", ny)
    ob = lax.ppermute(oa, "core", swap)
    full = (obs, members)
    wide, slim = pltpu.VMEM(full, f32), pltpu.VMEM(full, bf16)
    where = scalars(lax.axis_index("zl"), lax.axis_index("y"), core, first)
    return call(
        functools.partial(main_kernel, (bin_rows, nzl, ny)),
        jax.ShapeDtypeStruct(state.shape, f32),
        (where, par, oa, ob, na, nb, state),
        scratch=([slim] * 4 + [wide] * 3 + [slim] * 6 + [pltpu.VMEM((8, obs), f32)]
                 + [wide] * 4 + [slim] * 5),
        flops=20 << 30, room=32)


def solution(mesh):
    split = Mesh(mesh.devices.reshape(4, 2, 2, 4, 4), ROW_COL)
    placed = (P(None, ROW_COL), P(), P(), P(), P(None, None, COL))

    return jax.shard_map(
        on_device, mesh=split, in_specs=placed, out_specs=P(None, ROW_COL), check_vma=False
    )
```

```python
import functools

import jax
import jax.numpy as jnp
from jax import lax
from jax.experimental import pallas as pl
from jax.experimental.pallas import tpu as pltpu
from jax.sharding import Mesh
from jax.sharding import PartitionSpec as P


POSITIONS = 256
RADIUS = 64
ROW = ("x", "zh", "core")
COL = ("zl", "y")
ROW_COL = ROW + COL
SLOTS = 4

f32 = jnp.float32
bf16 = jnp.bfloat16
i32 = jnp.int32


def nn(a, b):
    return lax.dot_general(a, b, (((1,), (0,)), ((), ())), preferred_element_type=f32)


def nt(a, b):
    return lax.dot_general(a, b, (((1,), (1,)), ((), ())), preferred_element_type=f32)


def split2(x):
    high = x.astype(bf16)
    return high, (x - high.astype(f32)).astype(bf16)


def split3(x):
    high = x.astype(bf16)
    rest = x - high.astype(f32)
    middle = rest.astype(bf16)
    return high, middle, (rest - middle.astype(f32)).astype(bf16)


def one_hot(mask):
    return jnp.where(mask, 1.0, 0.0).astype(bf16)


def exact_nn(hot, x):
    high, middle, low = split3(x)
    return nn(hot, high) + nn(hot, middle) + nn(hot, low)


def exact_nt(hot, x):
    high, middle, low = split3(x)
    return nt(hot, high) + nt(hot, middle) + nt(hot, low)


def column_of(row):
    return jnp.broadcast_to(row, (128, row.shape[1])).T[:, 0:1]


def iota(shape, dim):
    return lax.broadcasted_iota(i32, shape, dim)


def shift_of(value):
    assert value & (value - 1) == 0
    return value.bit_length() - 1


def right(value, bits):
    return lax.shift_right_logical(value, jnp.full(jnp.shape(value), bits, i32))


def order_of(rows, tile_rows, obs):
    tile = right(rows, shift_of(tile_rows))
    key = (tile * obs + iota((1, obs), 1)).astype(f32)
    rank = jnp.sum(jnp.where(column_of(key) < key, 1.0, 0.0), axis=0, keepdims=True)
    rank = rank.astype(i32)
    return tile, rank


def par_kernel(dims, where_ref, index_ref, values_ref, var_ref, noise_ref, par_ref, noise_out_ref):
    bin_rows, tile_rows, cols = dims
    batches, obs = index_ref.shape
    for b in range(batches):
        rows = index_ref[b:b + 1, :]
        _, rank = order_of(rows, tile_rows, obs)
        placed = (rank & (cols - 1)) * (obs // cols) + right(rank, shift_of(cols))
        hot = one_hot(iota((obs, obs), 0) == placed)
        par = jnp.concatenate(
            [right(rows, shift_of(bin_rows)).astype(f32), values_ref[b:b + 1, :],
             var_ref[b:b + 1, :], jnp.zeros((13, obs), f32), noise_ref[b]], axis=0)
        count = par.shape[0]
        moved = nt(jnp.concatenate(split3(par), axis=0), hot)
        moved = moved[0:count] + moved[count:2 * count] + moved[2 * count:]
        par_ref[4 * b:4 * b + 4, :] = moved[0:4]
        noise_out_ref[b] = moved[16:]


def send_kernel(dims, where_ref, index_ref, state_ref, send_ref):
    tile_rows, _, cols = dims
    _, rows_dev = state_ref.shape
    batches, obs = index_ref.shape
    my_tile, first = where_ref[0], where_ref[1]
    slots = send_ref.shape[0]
    per_col = slots // cols
    pick = jnp.zeros((slots, rows_dev), f32)
    for b in range(batches):
        rows = index_ref[b:b + 1, :]
        tile, rank = order_of(rows, tile_rows, obs)
        col = rank & (cols - 1)
        start = jnp.sum(jnp.where(tile < my_tile, 1.0, 0.0), axis=1, keepdims=True).astype(i32)
        base = start + ((col - start) & (cols - 1))
        place = right(rank - base + cols * obs, shift_of(cols)) - obs
        local = rows - first
        inside = (local >= 0) & (local < rows_dev) & (place >= 0) & (place < SLOTS)
        slot = jnp.where(inside, col * per_col + b * SLOTS + place, -1)
        pick += nt(one_hot(iota((slots, obs), 0) == slot),
                   one_hot(iota((rows_dev, obs), 0) == local))
    send_ref[...] = exact_nt(pick.astype(bf16), state_ref[...])


def dense_kernel(dims, where_ref, index_ref, state_ref, send_ref):
    tile_rows, _, cols, each_row = dims
    _, rows_dev = state_ref.shape
    batches, obs = index_ref.shape
    width = 128
    spots = []
    for b in range(batches):
        rows = index_ref[b:b + 1, :]
        _, rank = order_of(rows, tile_rows, obs)
        item = b * (obs // cols) + right(rank, shift_of(cols))
        spot = right(item, shift_of(each_row)) * (cols * each_row)
        spot = spot + (rank & (cols - 1)) * each_row + (item & (each_row - 1))
        spots.append((spot, one_hot(iota((rows_dev, obs), 0) == rows - where_ref[1])))

    def part(ds, at, carry):
        pick = jnp.zeros((width, rows_dev), f32)
        for spot, local in spots:
            pick += nt(one_hot(iota((width, obs), 0) + at == spot), local)
        send_ref[ds, :] = exact_nt(pick.astype(bf16), state_ref[...])
        return carry

    pieces(send_ref.shape[0], width, part)


def place_kernel(dims, where_ref, index_ref, slots_ref, out_ref):
    tile_rows, cols, sizes = dims
    batches, _ = index_ref.shape
    slots = slots_ref.shape[0]
    my_col = where_ref[0]
    mine = [where_ref[1 + k] for k in range(3)]
    half = out_ref.shape[0] // batches
    p = iota((slots, 1), 0)
    block = right(p, shift_of(batches * SLOTS))
    batch = right(p, shift_of(SLOTS)) & (batches - 1)
    slot = p & (SLOTS - 1)
    nx, nz, nc = sizes
    block_z = block & (nz - 1)
    block_x = right(block, shift_of(nz)) & (nx - 1)
    block_c = right(block, shift_of(nz * nx))
    tile_p = (((mine[0] - block_x) & (nx - 1)) * nz + ((mine[1] - block_z) & (nz - 1))) * nc
    tile_p = tile_p + ((mine[2] - block_c) & (nc - 1))
    start = jnp.zeros((slots, 1), i32)
    end = jnp.zeros((slots, 1), i32)
    for b in range(batches):
        tile = right(index_ref[b:b + 1, :], shift_of(tile_rows))
        before = jnp.sum(jnp.where(tile < tile_p, 1.0, 0.0), axis=1, keepdims=True).astype(i32)
        through = jnp.sum(jnp.where(tile <= tile_p, 1.0, 0.0), axis=1, keepdims=True).astype(i32)
        start = jnp.where(batch == b, before, start)
        end = jnp.where(batch == b, through, end)
    rank = start + ((my_col - start) & (cols - 1)) + slot * cols
    j = right(rank - my_col, shift_of(cols)) - mine[2] * half
    target = jnp.where((rank < end) & (j >= 0) & (j < half), batch * half + j, -1)
    wide = 128
    hot = jnp.where(iota((slots, wide), 1) == target, 1.0, 0.0).T.astype(bf16)
    out_ref[...] = exact_nn(hot[0:out_ref.shape[0]], slots_ref[...])


def taper(first, second):
    scaled = (first - second) * (1.0 / RADIUS)
    return jnp.exp(-0.5 * scaled * scaled)


def put_in_place(where, source_a, source_b, target, skip, stride, nzl, ny):
    zl, y, core = where
    unit = target.shape[0] // (2 * nzl * ny)

    for k in range(nzl * ny):
        dy, dz = divmod(k, nzl)
        at = ((zl - dz) & (nzl - 1)) * ny + ((y - dy) & (ny - 1))
        begin = (k * stride + skip) * unit
        for source, half in ((source_a, core), (source_b, 1 - core)):
            to = pl.multiple_of((at * 2 + half) * unit, unit)
            target[pl.ds(to, unit), :] = source[begin:begin + unit, :]


def pieces(size, width, body, carry=0):
    def step(k, carry):
        at = k * width
        return body(pl.ds(pl.multiple_of(at, width), width), at, carry)

    return lax.fori_loop(0, size // width, step, carry)


def loop(size, width, body):
    def step(ds, at, carry):
        body(ds, at)
        return carry

    pieces(size, width, step)


def each(size, width, body):
    for at in range(0, size, width):
        body(slice(at, at + width), at)


def eye_part(obs, width, at):
    return iota((obs, width), 0) == iota((obs, width), 1) + at


def ident_part(obs, width, at):
    return jnp.where(eye_part(obs, width, at), 1.0, 0.0)


def centre(o, high, middle):
    def rows(ds, at):
        part = o[ds, :]
        part = part - jnp.mean(part, axis=1, keepdims=True)
        high[ds, :], middle[ds, :] = split2(part)

    each(o.shape[0], 128, rows)


def invert(pos_r, var_r, pos_c, members, high, middle, left, gram, other, spare, s_high, s_low,
           xa, xb, ra, rb, eh, vec):
    obs = gram.shape[0]
    width = obs
    norming = 1.0 / (members - 1)

    def cross_terms(ds, at):
        left[:, ds] = nt(high[...], middle[ds, :])

    each(obs, width, cross_terms)

    def covariance(ds, at):
        product = nt(high[...], high[ds, :]) + left[:, ds] + left[ds, :].T
        eye = eye_part(obs, width, at)
        covar = taper(pos_c, pos_r[:, ds]) * product * norming + jnp.where(eye, var_r[:, ds], 0.0)
        gram[:, ds] = covar
        vec[0:1, ds] = lax.rsqrt(jnp.sum(jnp.where(eye, covar, 0.0), axis=0, keepdims=True))

    each(obs, width, covariance)
    scale_c = column_of(vec[0:1, :])

    def rescale(ds, at):
        scaled = gram[:, ds] * scale_c * vec[0:1, ds]
        gram[:, ds] = scaled
        s_high[:, ds], s_low[:, ds] = split2(scaled)

    each(obs, 128, rescale)

    def squared(ds, at):
        square = nn(s_high[...], s_high[:, ds])
        left[:, ds] = square
        vec[1:2, ds] = jnp.sum(jnp.abs(square), axis=0, keepdims=True)

    each(obs, width, squared)
    upper = jnp.sqrt(jnp.max(vec[1:2, :], axis=1, keepdims=True)) * 1.01
    lower = jnp.min(var_r[...] * vec[0:1, :] * vec[0:1, :], axis=1, keepdims=True)
    alpha = 2.0 / (upper + lower)

    def widen(low_end):
        image = low_end * (2.0 - low_end)
        factor = 2.0 / (1.0 + image)
        return factor, factor * image

    factor, low_end = widen(alpha * lower)

    def first(ds, at):
        ident = ident_part(obs, 128, at)
        step = alpha * gram[:, ds]
        xa[:, ds] = (factor * alpha * (2.0 * ident - step)).astype(bf16)
        ra[:, ds] = (ident - factor * (2.0 * step - alpha * alpha * left[:, ds])).astype(bf16)

    each(obs, 128, first)

    def grow(old, new, factor):
        def part(ds, at):
            new[:, ds] = (factor * (old[:, ds].astype(f32) + nn(old[...], ra[:, ds]))).astype(bf16)

        each(obs, width, part)

    def remain(new):
        def part(ds, at):
            ra[:, ds] = (ident_part(obs, width, at) - nn(s_high[...], new[:, ds])).astype(bf16)

        each(obs, width, part)

    factor, low_end = widen(low_end)
    grow(xa, xb, factor)
    remain(xb)
    factor, low_end = widen(low_end)
    grow(xb, xa, factor)
    remain(xa)
    factor, low_end = widen(low_end)
    grow(xa, xb, factor)

    def remain_last(ds, at):
        residual = (ident_part(obs, width, at)
                    - nn(s_high[...], xb[:, ds]) - nn(s_low[...], xb[:, ds]))
        left[:, ds] = residual
        ra[:, ds] = residual.astype(bf16)
        vec[1:2, ds] = jnp.sum(jnp.abs(residual), axis=0, keepdims=True)

    each(obs, width, remain_last)

    def second_order(ds, at):
        rb[:, ds] = (left[:, ds] + nn(ra[...], ra[:, ds])).astype(bf16)

    each(obs, width, second_order)

    def correction(ds, at):
        eh[:, ds] = nn(xb[...], rb[:, ds]).astype(bf16)

    each(obs, width, correction)
    size = jnp.max(vec[1:2, :], axis=1, keepdims=True)

    @pl.when(jnp.logical_not(size[0, 0] < 0.1))
    def _():
        narrow = 128
        full = functools.partial(jnp.dot, precision=lax.Precision.HIGHEST,
                                 preferred_element_type=f32)
        sums = jnp.sum(jnp.abs(gram[...]), axis=0, keepdims=True)
        guess = 1.0 / jnp.max(sums, axis=1, keepdims=True)

        def start(ds, at):
            left[:, ds] = ident_part(obs, narrow, at) * guess

        loop(obs, narrow, start)

        def blocks(body, carry):
            def across(ds, at, carry):
                return pieces(obs, narrow, lambda dr, ar, c: body(dr, ar, ds, at, c), carry)

            return pieces(obs, narrow, across, carry)

        def advance(carry):
            def residuals(dr, ar, ds, at, error):
                eye = iota((narrow, narrow), 0) + ar == iota((narrow, narrow), 1) + at
                residual = jnp.where(eye, 1.0, 0.0) - full(gram[dr, :], left[:, ds])
                other[dr, ds] = residual
                return error + jnp.sum(residual * residual)

            def update(dr, ar, ds, at, carry):
                spare[dr, ds] = left[dr, ds] + full(left[dr, :], other[:, ds])
                return carry

            error = blocks(residuals, jnp.float32(0.0))
            blocks(update, 0)
            left[...] = spare[...]
            return carry[0] + 1, error

        lax.while_loop(lambda c: (c[0] < 40) & jnp.logical_not(c[1] < 1e-7), advance,
                       (jnp.int32(0), jnp.float32(1.0)))
        xb[...] = left[...].astype(bf16)
        eh[...] = (left[...] - xb[...].astype(f32)).astype(bf16)


def innovate(val_r, var_r, scale_r, o, n, vh, vl):
    deviation = jnp.sqrt(var_r)

    def rows(ds, at):
        part = val_r + deviation * n[ds, :] - o[:, ds].T
        vh[ds, :], vl[ds, :] = split2(part * scale_r)

    each(n.shape[0], 128, rows)


def weigh(pos_c, pos_dev, x, high, middle, members):
    xh, xl = split2(x - jnp.mean(x, axis=0, keepdims=True))
    cross = nn(high[...], xh) + nn(high[...], xl) + nn(middle[...], xh)
    return taper(pos_c, pos_dev) * cross * (1.0 / (members - 1))


def columns(par_ref):
    return jnp.concatenate([par_ref[...], jnp.zeros((120, par_ref.shape[1]), f32)], axis=0).T


def own_positions(first, rows_dev, bin_rows):
    return right(first + iota((1, rows_dev), 1), shift_of(bin_rows)).astype(f32)


def main_kernel(dims, where_ref, par_ref, oa, ob, na, nb, x_ref, out_ref,
                high0, middle0, high, middle, o0, o, n, vh, vl, sh, sl, xb, eh, vec, *work):
    bin_rows, nzl, ny = dims
    where = [where_ref[k] for k in range(3)]
    obs, members = o.shape
    left, gram, other, spare, s_high, s_low, xa, ra, rb = work
    cols_par = columns(par_ref)
    pos_dev = own_positions(where_ref[3], x_ref.shape[1], bin_rows)
    norming = 1.0 / (members - 1)
    put_in_place(where, oa, ob, o0, 0, 2, nzl, ny)
    put_in_place(where, na, nb, n, 0, 2, nzl, ny)
    pos_c = cols_par[:, 0:1]
    centre(o0, high0, middle0)
    invert(par_ref.at[0:1], par_ref.at[2:3], pos_c, members, high0, middle0, left, gram,
           other, spare, s_high, s_low, xa, xb, ra, rb, eh, vec)
    innovate(par_ref[1:2, :], par_ref[2:3, :], vec[0:1, :], o0, n, vh, vl)
    solved = nn(vh[...], xb[...]) + nn(vl[...], xb[...]) + nn(vh[...], eh[...])
    sh[...], sl[...] = split2(solved * vec[0:1, :])
    wh, wl = split2(weigh(pos_c, pos_dev, x_ref[...], high0, middle0, members))
    out_ref[...] = x_ref[...] + nn(sh[...], wh) + nn(sh[...], wl) + nn(sl[...], wh)
    put_in_place(where, oa, ob, o, 1, 2, nzl, ny)
    put_in_place(where, na, nb, n, 1, 2, nzl, ny)
    pos_c = cols_par[:, 4:5]
    centre(o, high, middle)

    def weights(ds, at):
        cross = nt(high[...], high0[ds, :]) + nt(high[...], middle0[ds, :])
        cross = cross + nt(middle[...], high0[ds, :])
        xa[:, ds], xb[:, ds] = split2(taper(pos_c, par_ref[0:1, ds]) * cross * norming)

    each(obs, obs, weights)

    def update(ds, at):
        o[:, ds] = (o[:, ds] + nt(xa[...], sh[ds, :]) + nt(xa[...], sl[ds, :])
                    + nt(xb[...], sh[ds, :]))

    each(members, members, update)
    centre(o, high, middle)
    invert(par_ref.at[4:5], par_ref.at[6:7], pos_c, members, high, middle, left, gram, other,
           spare, s_high, s_low, xa, xb, ra, rb, eh, vec)
    scale_c = column_of(vec[0:1, :])
    wh, wl = split2(weigh(pos_c, pos_dev, out_ref[...], high, middle, members) * scale_c)
    applied = nn(xb[...], wh) + nn(xb[...], wl) + nn(eh[...], wh)
    wh, wl = split2(applied * scale_c)
    innovate(par_ref[5:6, :], par_ref[6:7, :], jnp.ones((1, obs), f32), o, n, vh, vl)
    out_ref[...] = out_ref[...] + nn(vh[...], wh) + nn(vh[...], wl) + nn(vl[...], wh)


def ring_gather(value, axis, size):
    parts = [value]
    for k in range(1, size):
        parts.append(lax.ppermute(value, axis, [(i, (i + k) % size) for i in range(size)]))
    return jnp.concatenate(parts, axis=0)


def on_device(state, obs_index, obs_values, obs_var, noise):
    members, rows_dev = state.shape
    batches, obs = obs_index.shape
    cols = lax.axis_size(COL)
    nx, nz, nc = (lax.axis_size(a) for a in ROW)
    nzl, ny = (lax.axis_size(a) for a in COL)
    my_col = lax.axis_index(COL)
    my_tile = lax.axis_index(ROW)
    tile_rows = rows_dev * cols
    bin_rows = tile_rows * nx * nz * nc // POSITIONS
    first = (my_tile * cols + my_col) * rows_dev
    core = lax.axis_index("core")
    noise = jnp.swapaxes(noise, 1, 2)
    slots = cols * batches * SLOTS
    unit = obs // cols // nc
    prep_dims = (tile_rows, bin_rows, cols)

    def scalars(*values):
        return jnp.stack([jnp.asarray(v, i32) for v in values])

    smem = pl.BlockSpec(memory_space=pltpu.SMEM)
    vmem = pl.BlockSpec(memory_space=pltpu.VMEM)

    def call(kernel, shapes, inputs, scratch=(), flops=0, room=16):
        return pl.pallas_call(
            kernel,
            out_shape=shapes,
            in_specs=[smem] + [vmem] * (len(inputs) - 1),
            out_specs=jax.tree.map(lambda _: vmem, shapes),
            scratch_shapes=list(scratch),
            cost_estimate=pl.CostEstimate(flops=flops, bytes_accessed=4 << 20, transcendentals=0),
            compiler_params=pltpu.CompilerParams(vmem_limit_bytes=room << 20),
        )(*inputs)

    send = call(
        functools.partial(send_kernel, prep_dims),
        jax.ShapeDtypeStruct((slots, members), f32),
        (scalars(my_tile, first), obs_index, state), flops=1 << 28)
    mine = lax.all_to_all(send.reshape(cols, batches * SLOTS, members), COL, 0, 0, tiled=True)
    par, noise_t = call(
        functools.partial(par_kernel, (bin_rows, tile_rows, cols)),
        (jax.ShapeDtypeStruct((4 * batches, obs), f32),
         jax.ShapeDtypeStruct(noise.shape, f32)),
        (scalars(0), obs_index, obs_values, obs_var, noise), flops=1 << 30)
    mine = jnp.sum(mine, axis=0)
    mine = ring_gather(mine, "zh", nz)
    mine = ring_gather(mine, "x", nx)
    mine = ring_gather(mine, "core", nc)
    held = call(
        functools.partial(place_kernel, (tile_rows, cols, (nx, nz, nc))),
        jax.ShapeDtypeStruct((batches * unit, members), f32),
        (scalars(my_col, *(lax.axis_index(a) for a in ROW)), obs_index, mine),
        flops=1 << 28)

    def dense(held):
        tiles_all = nx * nz * nc
        each_row = batches * obs // cols // tiles_all
        send = call(
            functools.partial(dense_kernel, prep_dims + (each_row,)),
            jax.ShapeDtypeStruct((batches * obs, members), f32),
            (scalars(my_tile, first), obs_index, state))
        mine = lax.all_to_all(
            send.reshape(tiles_all * cols, each_row, members), ROW_COL, 0, 0, tiled=True)
        mine = jnp.sum(mine, axis=0)
        copies = jnp.broadcast_to(mine, (tiles_all, *mine.shape))
        mine = lax.all_to_all(copies, ROW, 0, 0, tiled=True)
        mine = mine.reshape(batches, nc, unit, members)
        return lax.dynamic_index_in_dim(mine, core, 1, keepdims=False).reshape(held.shape)

    tiles = obs_index[:, :, None] // tile_rows == jnp.arange(nx * nz * nc, dtype=i32)
    crowded = jnp.max(jnp.sum(tiles.astype(i32), axis=1)) > cols * SLOTS
    held = lax.cond(crowded, dense, lambda held: held, held)

    swap = [(0, 1), (1, 0)]
    part = noise.shape[1] // nc
    noise_half = lax.dynamic_slice_in_dim(noise_t, core * part, part, axis=1)
    na = ring_gather(noise_half.reshape(batches * part, obs), "zl", nzl)
    na = ring_gather(na, "y", ny)
    nb = lax.ppermute(na, "core", swap)
    oa = ring_gather(held, "zl", nzl)
    oa = ring_gather(oa, "y", ny)
    ob = lax.ppermute(oa, "core", swap)
    full = (obs, members)
    wide, slim = pltpu.VMEM(full, f32), pltpu.VMEM(full, bf16)
    where = scalars(lax.axis_index("zl"), lax.axis_index("y"), core, first)
    return call(
        functools.partial(main_kernel, (bin_rows, nzl, ny)),
        jax.ShapeDtypeStruct(state.shape, f32),
        (where, par, oa, ob, na, nb, state),
        scratch=([slim] * 4 + [wide] * 3 + [slim] * 6 + [pltpu.VMEM((8, obs), f32)]
                 + [wide] * 4 + [slim] * 5),
        flops=20 << 30, room=32)


def solution(mesh):
    split = Mesh(mesh.devices.reshape(4, 2, 2, 4, 4), ROW_COL)
    placed = (P(None, ROW_COL), P(), P(), P(), P(None, None, COL))

    return jax.shard_map(
        on_device, mesh=split, in_specs=placed, out_specs=P(None, ROW_COL), check_vma=False
    )
```
